32 devices in a mesh: dp: 32 (over z, y, x, core).
Axes of the slice: x: 2, y: 2, z: 4, core: 2. Of those that a mesh axis runs over, the one named last changes fastest.
Arguments:
- x_saved: bfloat16 [192, 64, 2048], P('dp')
- grad_out: bfloat16 [192, 64, 2048], P('dp')
- positions: int32 [192, 64], P('dp')
- attn_gain: bfloat16 [2048], replicated
- w_query: bfloat16 [2048, 32, 64], replicated
- w_key: bfloat16 [2048, 4, 64], replicated
- w_value: bfloat16 [2048, 4, 64], replicated
- w_out: bfloat16 [32, 64, 2048], replicated
- mlp_gain: bfloat16 [2048], replicated
- w_gate: bfloat16 [2048, 5632], replicated
- w_up: bfloat16 [2048, 5632], replicated
- w_down: bfloat16 [5632, 2048], replicated
- master_flat: float32 [44044288], P('dp')
- adam_mean: float32 [44044288], P('dp')
- adam_var: float32 [44044288], P('dp')
Outputs:
- output 1: bfloat16 [192, 64, 2048], P('dp')
- output 2: bfloat16 [2048], replicated
- output 3: bfloat16 [2048, 32, 64], replicated
- output 4: bfloat16 [2048, 4, 64], replicated
- output 5: bfloat16 [2048, 4, 64], replicated
- output 6: bfloat16 [32, 64, 2048], replicated
- output 7: bfloat16 [2048], replicated
- output 8: bfloat16 [2048, 5632], replicated
- output 9: bfloat16 [2048, 5632], replicated
- output 10: bfloat16 [5632, 2048], replicated
- output 11: float32 [44044288], P('dp')
- output 12: float32 [44044288], P('dp')
- output 13: float32 [44044288], P('dp')
- output 14: float32 [], replicated
All inputs are finite; a program needn't handle non-finite values.
Results may differ from the reference program's by a relative error of at most 0.0160587.
Values are sent between devices in bfloat16 or wider.
A program may use at most 1 GiB of HBM per device.

```python
import math
import jax
import jax.numpy as jnp
from jax import lax

MODEL_DIM = 2048
NUM_HEADS = 32
KV_HEADS = 4
HEAD_DIM = 64
FFN_DIM = 5632
SEQ_LEN = 64
SEQS_DEV = 6
DP_SIZE = 32
STEP_COUNT = 100
TOTAL_SEQS = SEQS_DEV * DP_SIZE
NPARAM = MODEL_DIM * (2 + 2 * HEAD_DIM * (NUM_HEADS + KV_HEADS) + 3 * FFN_DIM)
NORM_EPS = 1e-5
ROPE_BASE = 10000.0
LEARN_RATE = 2e-3
BETA_ONE = 0.9
BETA_TWO = 0.95
ADAM_EPS = 1e-8
WEIGHT_DECAY = 0.1


def param_shapes():
    return [(MODEL_DIM,), (MODEL_DIM, NUM_HEADS, HEAD_DIM), (MODEL_DIM, KV_HEADS, HEAD_DIM),
            (MODEL_DIM, KV_HEADS, HEAD_DIM), (NUM_HEADS, HEAD_DIM, MODEL_DIM), (MODEL_DIM,),
            (MODEL_DIM, FFN_DIM), (MODEL_DIM, FFN_DIM), (FFN_DIM, MODEL_DIM)]


def draw_params(key):
    key_list = jax.random.split(key, 9)
    fan_ins = [0, MODEL_DIM, MODEL_DIM, MODEL_DIM, NUM_HEADS * HEAD_DIM, 0, MODEL_DIM, MODEL_DIM, FFN_DIM]
    drawn_list = []
    for number, piece_shape in enumerate(param_shapes()):
        noise_arr = jax.random.normal(key_list[number], piece_shape, jnp.float32)
        if fan_ins[number] == 0:
            drawn_list.append(1.0 + 0.2 * noise_arr)
        else:
            drawn_list.append(noise_arr * fan_ins[number] ** -0.5)
    return drawn_list


def setup_inputs(seed: int = 0) -> dict:
    key_list = jax.random.split(jax.random.key(seed), 8)
    act_shape = (TOTAL_SEQS, SEQ_LEN, MODEL_DIM)
    x_saved = jax.random.normal(key_list[0], act_shape, jnp.float32).astype(jnp.bfloat16)
    grad_out = jax.random.normal(key_list[1], act_shape, jnp.float32).astype(jnp.bfloat16)
    pos_gaps = jax.random.randint(key_list[2], (TOTAL_SEQS, SEQ_LEN), 1, 4)
    positions = (jnp.cumsum(pos_gaps, axis=1) - 1).astype(jnp.int32)
    weights = [w_piece.astype(jnp.bfloat16) for w_piece in draw_params(key_list[3])]
    master_flat = jnp.concatenate([w_piece.reshape(-1) for w_piece in draw_params(key_list[4])])
    state_scale = NPARAM ** -0.5
    adam_mean = 0.1 * state_scale * jax.random.normal(key_list[5], (NPARAM,), jnp.float32)
    var_root = 0.3 * state_scale * jax.random.uniform(key_list[6], (NPARAM,), jnp.float32, 0.5, 1.5)
    adam_var = var_root * var_root
    return {'x_saved': x_saved, 'grad_out': grad_out, 'positions': positions,
            'attn_gain': weights[0], 'w_query': weights[1], 'w_key': weights[2], 'w_value': weights[3],
            'w_out': weights[4], 'mlp_gain': weights[5], 'w_gate': weights[6], 'w_up': weights[7],
            'w_down': weights[8], 'master_flat': master_flat, 'adam_mean': adam_mean, 'adam_var': adam_var}


def rms_scale(values, gain):
    wide = values.astype(jnp.float32)
    inv_rms = lax.rsqrt(jnp.mean(wide * wide, axis=-1, keepdims=True) + NORM_EPS)
    return (wide * inv_rms * gain.astype(jnp.float32)).astype(jnp.bfloat16)


def rope_tables(positions, head_dim):
    half_dim = head_dim // 2
    inv_freq = ROPE_BASE ** (-2.0 * jnp.arange(half_dim, dtype=jnp.float32) / head_dim)
    angles = positions.astype(jnp.float32)[:, :, None] * inv_freq
    cos_full = jnp.concatenate([jnp.cos(angles), jnp.cos(angles)], axis=-1)[:, :, None, :]
    sin_full = jnp.concatenate([jnp.sin(angles), jnp.sin(angles)], axis=-1)[:, :, None, :]
    return cos_full, sin_full


def rope_apply(values, cos_full, sin_full):
    half_dim = values.shape[-1] // 2
    rotated = jnp.concatenate([-values[..., half_dim:], values[..., :half_dim]], axis=-1)
    return values * cos_full + rotated * sin_full


def layer_forward(w_list, x_val, positions):
    attn_gain, w_query, w_key, w_value, w_out, mlp_gain, w_gate, w_up, w_down = w_list
    num_seqs, seq_len, model_dim = x_val.shape
    num_heads, head_dim = w_query.shape[1], w_query.shape[2]
    kv_heads = w_key.shape[1]
    group_size = num_heads // kv_heads
    n_tok = num_seqs * seq_len
    x_flat = x_val.reshape(n_tok, model_dim)
    normed = rms_scale(x_flat, attn_gain)
    q_pre = jnp.dot(normed, w_query.reshape(model_dim, num_heads * head_dim), preferred_element_type=jnp.float32)
    k_pre = jnp.dot(normed, w_key.reshape(model_dim, kv_heads * head_dim), preferred_element_type=jnp.float32)
    v_pre = jnp.dot(normed, w_value.reshape(model_dim, kv_heads * head_dim), preferred_element_type=jnp.float32)
    v_heads = v_pre.astype(jnp.bfloat16).reshape(num_seqs, seq_len, kv_heads, head_dim)
    cos_full, sin_full = rope_tables(positions, head_dim)
    q_rot = rope_apply(q_pre.reshape(num_seqs, seq_len, num_heads, head_dim), cos_full, sin_full).astype(jnp.bfloat16)
    q_rot = q_rot.reshape(num_seqs, seq_len, kv_heads, group_size, head_dim)
    k_rot = rope_apply(k_pre.reshape(num_seqs, seq_len, kv_heads, head_dim), cos_full, sin_full).astype(jnp.bfloat16)
    scores = jnp.einsum('bqkgd,bskd->bkgqs', q_rot.astype(jnp.float32), k_rot.astype(jnp.float32)) * head_dim ** -0.5
    causal = jnp.arange(seq_len)[:, None] >= jnp.arange(seq_len)[None, :]
    attn_probs = jax.nn.softmax(jnp.where(causal, scores, -1e30), axis=-1).astype(jnp.bfloat16)
    context = jnp.einsum('bkgqs,bskd->bqkgd', attn_probs.astype(jnp.float32), v_heads.astype(jnp.float32)).astype(jnp.bfloat16)
    attn_out = jnp.dot(context.reshape(n_tok, num_heads * head_dim), w_out.reshape(num_heads * head_dim, model_dim), preferred_element_type=jnp.float32)
    hidden = (x_flat.astype(jnp.float32) + attn_out).astype(jnp.bfloat16)
    normed_mlp = rms_scale(hidden, mlp_gain)
    gate_pre = jnp.dot(normed_mlp, w_gate, preferred_element_type=jnp.float32)
    up_pre = jnp.dot(normed_mlp, w_up, preferred_element_type=jnp.float32)
    gated_act = (jax.nn.silu(gate_pre) * up_pre).astype(jnp.bfloat16)
    down_out = jnp.dot(gated_act, w_down, preferred_element_type=jnp.float32)
    return (hidden.astype(jnp.float32) + down_out).astype(jnp.bfloat16).reshape(num_seqs, seq_len, model_dim)


def split_flat(flat_vec):
    pieces = []
    offset = 0
    for piece_shape in param_shapes():
        piece_size = math.prod(piece_shape)
        pieces.append(flat_vec[offset:offset + piece_size].reshape(piece_shape))
        offset += piece_size
    return pieces


def reference(x_saved, grad_out, positions, attn_gain, w_query, w_key, w_value, w_out, mlp_gain, w_gate, w_up, w_down, master_flat, adam_mean, adam_var):
    w_list = (attn_gain, w_query, w_key, w_value, w_out, mlp_gain, w_gate, w_up, w_down)

    def device_grads(grad_acc, group_in):
        x_group, dy_group, pos_group = group_in
        layer_out, pullback = jax.vjp(lambda x_val, w_vals: layer_forward(w_vals, x_val, pos_group), x_group, w_list)
        grad_x, grad_w = pullback(dy_group)
        flat_grad = jnp.concatenate([w_grad.astype(jnp.bfloat16).reshape(-1).astype(jnp.float32) for w_grad in grad_w])
        return grad_acc + flat_grad, grad_x.astype(jnp.bfloat16)

    group_shape = (DP_SIZE, SEQS_DEV, SEQ_LEN, MODEL_DIM)
    grad_sum, grad_x = lax.scan(device_grads, jnp.zeros((NPARAM,), jnp.float32),
                                (x_saved.reshape(group_shape), grad_out.reshape(group_shape),
                                 positions.reshape(DP_SIZE, SEQS_DEV, SEQ_LEN)))
    grad_mean = grad_sum / DP_SIZE
    grad_norm = jnp.sqrt(jnp.sum(grad_mean * grad_mean))
    clip_scale = jnp.minimum(1.0, 1.0 / (grad_norm + 1e-6))
    clipped = grad_mean * clip_scale
    new_mean = BETA_ONE * adam_mean + (1.0 - BETA_ONE) * clipped
    new_var = BETA_TWO * adam_var + (1.0 - BETA_TWO) * clipped * clipped
    mean_hat = new_mean / (1.0 - BETA_ONE ** STEP_COUNT)
    var_hat = new_var / (1.0 - BETA_TWO ** STEP_COUNT)
    gain_two = MODEL_DIM + 2 * MODEL_DIM * HEAD_DIM * (NUM_HEADS + KV_HEADS)
    flat_index = jnp.arange(NPARAM)
    is_gain = (flat_index < MODEL_DIM) | ((flat_index >= gain_two) & (flat_index < gain_two + MODEL_DIM))
    decays = jnp.where(is_gain, 0.0, WEIGHT_DECAY)
    new_master = master_flat - LEARN_RATE * (mean_hat / (jnp.sqrt(var_hat) + ADAM_EPS) + decays * master_flat)
    new_weights = split_flat(new_master.astype(jnp.bfloat16))
    return (grad_x.reshape(TOTAL_SEQS, SEQ_LEN, MODEL_DIM), new_weights[0], new_weights[1], new_weights[2],
            new_weights[3], new_weights[4], new_weights[5], new_weights[6], new_weights[7], new_weights[8],
            new_master, new_mean, new_var, grad_norm)
```

```python
import functools
import jax
import jax.numpy as jnp
import numpy as np
from jax import lax
from jax.experimental import pallas as pl
from jax.experimental.pallas import tpu as pltpu
from jax.sharding import PartitionSpec as P

NORM_EPS = 1e-5
ROPE_BASE = 10000.0
LEARN_RATE = 2e-3
BETA_ONE = 0.9
BETA_TWO = 0.95
ADAM_EPS = 1e-8
WEIGHT_DECAY = 0.1
STEP_COUNT = 100

MATS = ((2, 1), (4096, 16), (512, 2), (512, 2), (4096, 16), (2, 1), (11264, 44), (11264, 44), (11264, 16))
OFFS = tuple(int(o) for o in np.cumsum([0] + [m[0] for m in MATS]))
NDEV = 32
TILES = OFFS[-1]
ROWS = TILES * 8 // NDEV
HALO = 352
WIN_R = 1408
WIN_A = 1376
HALF = WIN_A // 2
S_ROWS = 11464
X_ROWS = 11112


def group_of(row):
    tile = row // 8
    mat = max(m for m in range(len(MATS)) if OFFS[m] <= tile)
    per = MATS[mat][1]
    return OFFS[mat] + (tile - OFFS[mat]) // per * per, per


def plan():
    lo, hi, own = [], [], []
    for dev in range(NDEV):
        start, per = group_of(ROWS * dev)
        last, last_per = group_of(ROWS * (dev + 1) - 1)
        lo.append(start)
        hi.append(last + last_per)
        own.append(start if start * 8 == ROWS * dev else start + per)
    own.append(TILES)
    return lo, hi, own


LO, HI, OWN = plan()
BASE = [min(a, TILES - WIN_R) for a in LO]


def overlap(a, b, mat):
    return max(a, OFFS[mat]), min(b, OFFS[mat + 1])


def tables():
    rows_in, rows_out = [], []
    for dev in range(NDEV):
        r_in, r_out = [], []
        for mat, (_, per) in enumerate(MATS):
            a, b = overlap(LO[dev], HI[dev], mat)
            n = max(0, b - a) // per
            r_in += [a - BASE[dev], 8 * a - ROWS * dev + HALO, n] if n else [0, 0, 0]
            a, b = overlap(OWN[dev], OWN[dev + 1], mat)
            n = max(0, b - a) // per
            r_out += [a - OWN[dev], 8 * a - ROWS * dev, n] if n else [0, 0, 0]
        rows_in.append(r_in)
        rows_out.append(r_out)
    return np.array(rows_in, np.int32), np.array(rows_out, np.int32)


def to_tiles(mat2d):
    rows, cols = mat2d.shape
    return mat2d.reshape(rows // 8, 8, cols // 128, 128).transpose(0, 2, 1, 3).reshape(-1, 8, 128)


def from_tiles(tiles, rows, cols):
    return tiles.reshape(rows // 8, cols // 128, 8, 128).transpose(0, 2, 1, 3).reshape(rows, cols)


def unpermute_kernel(tab, x_ref, o_ref):
    o_ref[0:HALO, :] = jnp.zeros((HALO, 128), jnp.float32)
    o_ref[S_ROWS - 376:S_ROWS, :] = jnp.zeros((376, 128), jnp.float32)
    for mat, (_, per) in enumerate(MATS):
        t0, r0 = tab[3 * mat], tab[3 * mat + 1]

        def body(g, carry, per=per, t0=t0, r0=r0):
            for j in range(per):
                o_ref[pl.ds(r0 + g * (8 * per) + j, 8, stride=per), :] = x_ref[t0 + g * per + j].astype(jnp.float32)
            return carry

        lax.fori_loop(0, tab[3 * mat + 2], body, 0)


def unpermute(tab, win):
    return pl.pallas_call(
        unpermute_kernel,
        out_shape=jax.ShapeDtypeStruct((S_ROWS, 128), jnp.float32),
        grid_spec=pltpu.PrefetchScalarGridSpec(
            num_scalar_prefetch=1, grid=(1,),
            in_specs=[pl.BlockSpec((WIN_R, 8, 128), lambda i, t: (0, 0, 0))],
            out_specs=pl.BlockSpec((S_ROWS, 128), lambda i, t: (0, 0))),
        compiler_params=pltpu.CompilerParams(vmem_limit_bytes=40 << 20),
        cost_estimate=pl.CostEstimate(flops=4000000, bytes_accessed=9000000, transcendentals=0),
    )(tab, win)


def permute_kernel(tab, x_ref, h_ref, o_ref, s_ref):
    def fill(k, carry):
        at = pl.ds(pl.multiple_of(k * 64, 64), 64)
        s_ref[at, :] = x_ref[at, :]
        return carry

    lax.fori_loop(0, ROWS // 64, fill, 0)
    s_ref[ROWS // 64 * 64:ROWS, :] = x_ref[ROWS // 64 * 64:ROWS, :]
    s_ref[ROWS:ROWS + HALO, :] = h_ref[...]
    for mat, (_, per) in enumerate(MATS):
        t0, r0 = tab[3 * mat], tab[3 * mat + 1]

        def body(g, carry, per=per, t0=t0, r0=r0):
            for j in range(per):
                o_ref[t0 + g * per + j] = s_ref[pl.ds(r0 + g * (8 * per) + j, 8, stride=per), :].astype(jnp.bfloat16)
            return carry

        lax.fori_loop(0, tab[3 * mat + 2], body, 0)


def permute(tab, rows, halo):
    return pl.pallas_call(
        permute_kernel,
        out_shape=jax.ShapeDtypeStruct((WIN_A, 8, 128), jnp.bfloat16),
        grid_spec=pltpu.PrefetchScalarGridSpec(
            num_scalar_prefetch=1, grid=(1,),
            in_specs=[pl.BlockSpec((ROWS, 128), lambda i, t: (0, 0)), pl.BlockSpec((HALO, 128), lambda i, t: (0, 0))],
            out_specs=pl.BlockSpec((WIN_A, 8, 128), lambda i, t: (0, 0, 0)),
            scratch_shapes=[pltpu.VMEM((X_ROWS, 128), jnp.float32)]),
        compiler_params=pltpu.CompilerParams(vmem_limit_bytes=40 << 20),
        cost_estimate=pl.CostEstimate(flops=4000000, bytes_accessed=9000000, transcendentals=0),
    )(tab, rows, halo)


def gather_kernel(x_ref, out_ref, own_sem, send_sem, recv_sem):
    me = lax.axis_index('dp')
    core, xx, yy, zz = me % 2, (me // 2) % 2, (me // 4) % 2, me // 8

    def dev(z, y, x, c):
        return ((z * 2 + y) * 2 + x) * 2 + c

    up, down = dev(zz + 1, yy, xx, core), dev(zz - 1, yy, xx, core)
    xn, yn, mate = dev(zz, yy, 1 - xx, core), dev(zz, 1 - yy, xx, core), dev(zz, yy, xx, 1 - core)
    has_up, has_down = zz < 3, zz > 0

    barrier = pltpu.get_barrier_semaphore()
    for target in (xn, yn, mate):
        pl.semaphore_signal(barrier, inc=1, device_id=(target,), device_id_type=pl.DeviceIdType.MESH)
    for cond, target in ((has_up, up), (has_down, down)):
        @pl.when(cond)
        def _(target=target):
            pl.semaphore_signal(barrier, inc=1, device_id=(target,), device_id_type=pl.DeviceIdType.MESH)
    pl.semaphore_wait(barrier, 3 + has_up.astype(jnp.int32) + has_down.astype(jnp.int32))

    sent = []

    def part(ref, h):
        return ref.at[pl.ds(h * HALF, HALF)]

    def copy(src, slot, h, target, k):
        return pltpu.make_async_remote_copy(
            src_ref=src, dst_ref=out_ref.at[slot, pl.ds(h * HALF, HALF)],
            send_sem=send_sem.at[k], recv_sem=recv_sem.at[slot, h],
            device_id=(target,), device_id_type=pl.DeviceIdType.MESH)

    def send(conds, src, slot, h, target):
        k = len(sent)
        desc = copy(src, slot, h, target, k)
        sent.append(conds)
        if conds[-1] is None:
            desc.start()
        else:
            @pl.when(conds[-1])
            def _():
                desc.start()

    def arrived(slot, h):
        copy(part(out_ref.at[slot], h), slot, h, mate, 0).wait_recv()

    own_copy = pltpu.make_async_copy(x_ref, out_ref.at[me], own_sem)
    own_copy.start()
    for h in range(2):
        src = part(x_ref, h)
        send((has_up,), src, me, h, up)
        send((has_down,), src, me, h, down)
        send((None,), src, me, h, xn)
        send((None,), src, me, h, yn)
    for h in range(2):
        send((None,), part(x_ref, h), me, h, mate)

    def column(step):
        if step == 0:
            return [(None, zz, None)]
        return [(zz - step >= 0, zz - step, 'up'), (zz + step <= 3, zz + step, 'down')]

    def guarded(cond, body):
        if cond is None:
            body()
        else:
            pl.when(cond)(body)

    for step in range(6):
        if 1 <= step <= 3:
            for cond, zs, way in column(step):
                def body(cond=cond, zs=zs, way=way):
                    slot = dev(zs, yy, xx, core)
                    for h in range(2):
                        arrived(slot, h)
                        src = part(out_ref.at[slot], h)
                        onward = has_up if way == 'up' else has_down
                        send((cond, onward), src, slot, h, up if way == 'up' else down)
                        send((cond, None), src, slot, h, xn)
                        send((cond, None), src, slot, h, yn)
                        send((cond, None), src, slot, h, mate)
                guarded(cond, body)
        if 1 <= step <= 4:
            for cond, zs, _ in column(step - 1):
                def body(cond=cond, zs=zs):
                    for h in range(2):
                        for side in range(2):
                            slot = dev(zs, yy, 1 - xx, core) if side == 0 else dev(zs, 1 - yy, xx, core)
                            arrived(slot, h)
                            src = part(out_ref.at[slot], h)
                            if h == side:
                                send((cond, None), src, slot, h, yn if side == 0 else xn)
                            send((cond, None), src, slot, h, mate)
                guarded(cond, body)
        if 2 <= step <= 5:
            for cond, zs, _ in column(step - 2):
                def body(cond=cond, zs=zs):
                    slot = dev(zs, 1 - yy, 1 - xx, core)
                    for h in range(2):
                        arrived(slot, h)
                        send((cond, None), part(out_ref.at[slot], h), slot, h, mate)
                guarded(cond, body)

    def drain(k, carry):
        slot = (k // 2) * 2 + (1 - core)
        out = out_ref.at[slot]
        for h in range(2):
            @pl.when(k % 2 == h)
            def _(h=h):
                arrived(slot, h)
        return carry

    lax.fori_loop(0, NDEV, drain, 0)
    for k, conds in enumerate(sent):
        conds = [c for c in conds if c is not None]
        wait_send = copy(part(x_ref, 0), me, 0, mate, k).wait_send
        if not conds:
            wait_send()
        else:
            cond = conds[0]
            for c in conds[1:]:
                cond = jnp.logical_and(cond, c)
            pl.when(cond)(wait_send)
    own_copy.wait()


def gather(shard):
    return pl.pallas_call(
        gather_kernel,
        out_shape=jax.ShapeDtypeStruct((NDEV, WIN_A, 8, 128), jnp.bfloat16),
        in_specs=[pl.BlockSpec(memory_space=pltpu.VMEM)],
        out_specs=pl.BlockSpec(memory_space=pl.ANY),
        scratch_shapes=[pltpu.SemaphoreType.DMA, pltpu.SemaphoreType.DMA((128,)), pltpu.SemaphoreType.DMA((NDEV, 2))],
        compiler_params=pltpu.CompilerParams(collective_id=1, has_side_effects=True, vmem_limit_bytes=16 << 20),
    )(shard)


HALF_R = WIN_R // 2
PIECES = ((1, 1, 0), (1, 1, 1), (1, 0, 0), (0, 1, 1), (0, 1, 0), (1, 0, 1), (0, 0, 0), (0, 0, 1))


def scatter_kernel(src_ref, out_ref, land_mate, land_one, land_two, land_z, acc, tmp,
                   load_sem, tmp_sem, out_sem, send_sem, mate_sem, one_sem, two_sem, z_sem):
    me = lax.axis_index('dp')
    core, xx, yy, zz = me % 2, (me // 2) % 2, (me // 4) % 2, me // 8

    def dev(z, y, x, c):
        return ((z * 2 + y) * 2 + x) * 2 + c

    xn, yn, mate = dev(zz, yy, 1 - xx, core), dev(zz, 1 - yy, xx, core), dev(zz, yy, xx, 1 - core)
    up, down = dev(zz + 1, yy, xx, core), dev(zz - 1, yy, xx, core)
    has_up, has_down = zz < 3, zz > 0

    barrier = pltpu.get_barrier_semaphore()
    for target in (xn, yn, mate):
        pl.semaphore_signal(barrier, inc=1, device_id=(target,), device_id_type=pl.DeviceIdType.MESH)
    for cond, target in ((has_up, up), (has_down, down)):
        @pl.when(cond)
        def _(target=target):
            pl.semaphore_signal(barrier, inc=1, device_id=(target,), device_id_type=pl.DeviceIdType.MESH)
    pl.semaphore_wait(barrier, 3 + has_up.astype(jnp.int32) + has_down.astype(jnp.int32))

    low = jnp.minimum(zz, 3 - zz)
    flip = zz >= 2
    order = []
    for far, near in ((3, 3), (2, 0), (1, 2)):
        at = jnp.where(low == 0, far, near)
        order.append(jnp.where(flip, 3 - at, at))
    order.append(zz)

    def remote(src, dst, send, recv, target):
        return pltpu.make_async_remote_copy(src_ref=src, dst_ref=dst, send_sem=send, recv_sem=recv,
                                            device_id=(target,), device_id_type=pl.DeviceIdType.MESH)

    def slot_half(k, piece, c):
        dy, dx, h = piece
        y = 1 - yy if dy else yy
        x = 1 - xx if dx else xx
        return src_ref.at[dev(order[k], y, x, c), pl.ds(h * HALF_R, HALF_R)]

    def index(k, piece):
        return k * 8 + PIECES.index(piece)

    def to_mate(k, piece):
        i = index(k, piece)
        return remote(slot_half(k, piece, 1 - core), land_mate.at[i], send_sem.at[i], mate_sem.at[i], mate)

    def load(k, piece):
        i = index(k, piece)
        return pltpu.make_async_copy(slot_half(k, piece, core), acc.at[i], load_sem.at[i])

    def hop_one(k, piece):
        j = k * 4 + (piece[1] if piece[2] == 0 else 2 + piece[0])
        return remote(acc.at[index(k, piece)], land_one.at[j], send_sem.at[32 + j], one_sem.at[j],
                      yn if piece[2] == 0 else xn)

    def hop_two(k, h):
        j = k * 2 + h
        piece = (0, 1, 0) if h == 0 else (1, 0, 1)
        return remote(acc.at[index(k, piece)], land_two.at[j], send_sem.at[48 + j], two_sem.at[j],
                      xn if h == 0 else yn)

    def hop_z(k, h, way):
        i = index(k, (0, 0, h))
        return remote(acc.at[i], land_z.at[way, order[k], h], send_sem.at[56 + k * 2 + h], z_sem.at[way, order[k], h],
                      down if way else up)

    def add(i, landed):
        copy = pltpu.make_async_copy(landed, tmp, tmp_sem)
        copy.start()
        copy.wait()

        def body(t, carry):
            at = pl.ds(pl.multiple_of(t * 16, 16), 16)
            acc[i, at] = (acc[i, at].astype(jnp.float32) + tmp[at].astype(jnp.float32)).astype(jnp.bfloat16)
            return carry

        lax.fori_loop(0, HALF_R // 16, body, 0)

    for k in range(4):
        for piece in PIECES:
            to_mate(k, piece).start()
            load(k, piece).start()

    def prepare(k):
        for piece in PIECES:
            i = index(k, piece)
            load(k, piece).wait()
            to_mate(k, piece).wait_recv()
            add(i, land_mate.at[i])
            if piece[piece[2]] == 1:
                hop_one(k, piece).start()

    def second(k):
        for h, piece in ((0, (0, 1, 0)), (1, (1, 0, 1))):
            j = k * 4 + (1 if h == 0 else 3)
            remote(tmp, land_one.at[j], send_sem.at[32 + j], one_sem.at[j], xn).wait_recv()
            add(index(k, piece), land_one.at[j])
            hop_two(k, h).start()

    def final(k):
        zs = order[k]
        for h in range(2):
            i = index(k, (0, 0, h))
            j = k * 4 + (0 if h == 0 else 2)
            remote(tmp, land_one.at[j], send_sem.at[32 + j], one_sem.at[j], xn).wait_recv()
            add(i, land_one.at[j])
        for h in range(2):
            i = index(k, (0, 0, h))
            hop_two(k, h).wait_recv()
            add(i, land_two.at[k * 2 + h])
            for way, cond in ((0, (zs >= zz) & has_down), (1, (zs <= zz) & has_up)):
                @pl.when(cond)
                def _(way=way, h=h, i=i):
                    hop_z(k, h, way).wait_recv()
                    add(i, land_z.at[way, zs, h])
            if k < 3:
                for way, cond in ((0, zs > zz), (1, zs < zz)):
                    @pl.when(cond)
                    def _(way=way, h=h):
                        hop_z(k, h, way).start()
            else:
                pltpu.make_async_copy(acc.at[i], out_ref.at[pl.ds(h * HALF_R, HALF_R)], out_sem.at[h]).start()

    prepare(0)
    prepare(1)
    second(0)
    prepare(2)
    second(1)
    prepare(3)
    final(0)
    second(2)
    final(1)
    second(3)
    final(2)
    final(3)
    for n in range(62):
        remote(tmp, land_mate.at[0], send_sem.at[n], mate_sem.at[0], mate).wait_send()
    for h in range(2):
        pltpu.make_async_copy(acc.at[index(3, (0, 0, h))], out_ref.at[pl.ds(h * HALF_R, HALF_R)], out_sem.at[h]).wait()


def scatter(slots):
    def lands(*lead):
        return jax.ShapeDtypeStruct(lead + (HALF_R, 8, 128), jnp.bfloat16)

    any_spec = pl.BlockSpec(memory_space=pl.ANY)
    dma = pltpu.SemaphoreType.DMA
    return pl.pallas_call(
        scatter_kernel,
        out_shape=(jax.ShapeDtypeStruct((WIN_R, 8, 128), jnp.bfloat16), lands(32), lands(16), lands(8), lands(2, 4, 2)),
        in_specs=[any_spec],
        out_specs=(any_spec,) * 5,
        scratch_shapes=[pltpu.VMEM((32, HALF_R, 8, 128), jnp.bfloat16), pltpu.VMEM((HALF_R, 8, 128), jnp.bfloat16),
                        dma((32,)), dma, dma((2,)), dma((62,)), dma((32,)), dma((16,)), dma((8,)), dma((2, 4, 2))],
        compiler_params=pltpu.CompilerParams(collective_id=2, has_side_effects=True, vmem_limit_bytes=56 << 20),
    )(slots)[0]


BUFS = 6


def move_kernel(moves, n_in, n_out, *refs):
    ins, outs = refs[:n_in], refs[n_in:n_in + n_out]
    buf, in_sem, out_sem = refs[n_in + n_out:]

    def read(n):
        src, a, _, _, count = moves[n]
        return pltpu.make_async_copy(ins[src].at[pl.ds(a, count)], buf.at[n % BUFS, pl.ds(0, count)], in_sem.at[n % BUFS])

    def write(n):
        _, _, dst, b, count = moves[n]
        return pltpu.make_async_copy(buf.at[n % BUFS, pl.ds(0, count)], outs[dst].at[pl.ds(b, count)], out_sem.at[n % BUFS])

    ahead = BUFS // 2
    for n in range(len(moves) + ahead):
        if n < len(moves):
            if n >= BUFS:
                write(n - BUFS).wait()
            read(n).start()
        if n >= ahead:
            read(n - ahead).wait()
            write(n - ahead).start()
    for n in range(max(0, len(moves) - BUFS), len(moves)):
        write(n).wait()


def move(moves, arrays, out_tiles):
    moves = tuple(m[:1] + (m[1] + c,) + m[2:3] + (m[3] + c, min(BLOCK, m[4] - c)) for m in moves for c in range(0, m[4], BLOCK))
    return pl.pallas_call(
        functools.partial(move_kernel, moves, len(arrays), len(out_tiles)),
        out_shape=tuple(jax.ShapeDtypeStruct((n, 8, 128), jnp.bfloat16) for n in out_tiles),
        in_specs=[pl.BlockSpec(memory_space=pl.ANY)] * len(arrays),
        out_specs=(pl.BlockSpec(memory_space=pl.ANY),) * len(out_tiles),
        scratch_shapes=[pltpu.VMEM((BUFS, BLOCK, 8, 128), jnp.bfloat16), pltpu.SemaphoreType.DMA((BUFS,)),
                        pltpu.SemaphoreType.DMA((BUFS,))],
        compiler_params=pltpu.CompilerParams(vmem_limit_bytes=20 << 20),
        cost_estimate=pl.CostEstimate(flops=100000000, bytes_accessed=176000000, transcendentals=0),
    )(*arrays)


BLOCK = 704


def rope_tables(positions, head_dim):
    half_dim = head_dim // 2
    inv_freq = ROPE_BASE ** (-2.0 * jnp.arange(half_dim, dtype=jnp.float32) / head_dim)
    angles = positions.astype(jnp.float32)[:, :, None] * inv_freq
    cos_full = jnp.concatenate([jnp.cos(angles), jnp.cos(angles)], axis=-1)[:, :, None, :]
    sin_full = jnp.concatenate([jnp.sin(angles), jnp.sin(angles)], axis=-1)[:, :, None, :]
    return cos_full, sin_full


def rope_apply(values, cos_full, sin_full):
    half_dim = values.shape[-1] // 2
    rotated = jnp.concatenate([-values[..., half_dim:], values[..., :half_dim]], axis=-1)
    return values * cos_full + rotated * sin_full


def rope_back(grad_rot, cos_full, sin_full):
    half_dim = grad_rot.shape[-1] // 2
    scaled = grad_rot * sin_full
    return grad_rot * cos_full + jnp.concatenate([scaled[..., half_dim:], -scaled[..., :half_dim]], axis=-1)


def rms_parts(values):
    inv_rms = lax.rsqrt(jnp.mean(values * values, axis=-1, keepdims=True) + NORM_EPS)
    return inv_rms, values * inv_rms


def rms_back(d_normed, gain_wide, inv_rms, x_hat):
    d_hat = d_normed * gain_wide
    return inv_rms * (d_hat - x_hat * jnp.mean(d_hat * x_hat, axis=-1, keepdims=True))


def local_grads(x_loc, dy_loc, pos_loc, w_list):
    attn_gain, w_query, w_key, w_value, w_out, mlp_gain, w_gate, w_up, w_down = w_list
    num_seqs, seq_len, model_dim = x_loc.shape
    num_heads, head_dim = w_query.shape[1], w_query.shape[2]
    kv_heads = w_key.shape[1]
    group_size = num_heads // kv_heads
    n_tok = num_seqs * seq_len
    wq_flat = w_query.reshape(model_dim, num_heads * head_dim)
    wk_flat = w_key.reshape(model_dim, kv_heads * head_dim)
    wv_flat = w_value.reshape(model_dim, kv_heads * head_dim)
    wo_flat = w_out.reshape(num_heads * head_dim, model_dim)
    dy_flat = dy_loc.reshape(n_tok, model_dim)
    x_wide = x_loc.reshape(n_tok, model_dim).astype(jnp.float32)
    inv_one, value_a8 = rms_parts(x_wide)
    gain_one = attn_gain.astype(jnp.float32)
    normed = (value_a8 * gain_one).astype(jnp.bfloat16)
    q_pre = jnp.dot(normed, wq_flat, preferred_element_type=jnp.float32).reshape(num_seqs, seq_len, num_heads, head_dim)
    k_pre = jnp.dot(normed, wk_flat, preferred_element_type=jnp.float32).reshape(num_seqs, seq_len, kv_heads, head_dim)
    v_heads = jnp.dot(normed, wv_flat, preferred_element_type=jnp.float32).astype(jnp.bfloat16).reshape(num_seqs, seq_len, kv_heads, head_dim)
    cos_full, sin_full = rope_tables(pos_loc, head_dim)
    q_rot = rope_apply(q_pre, cos_full, sin_full).astype(jnp.bfloat16).reshape(num_seqs, seq_len, kv_heads, group_size, head_dim)
    k_rot = rope_apply(k_pre, cos_full, sin_full).astype(jnp.bfloat16)
    score_scale = head_dim ** -0.5
    scores = jnp.einsum('bqkgd,bskd->bkgqs', q_rot, k_rot, preferred_element_type=jnp.float32) * score_scale
    causal = lax.iota(jnp.int32, seq_len)[:, None] >= lax.iota(jnp.int32, seq_len)[None, :]
    attn_probs = jax.nn.softmax(jnp.where(causal, scores, -1e30), axis=-1)
    probs_low = attn_probs.astype(jnp.bfloat16)
    context = jnp.einsum('bkgqs,bskd->bqkgd', probs_low, v_heads, preferred_element_type=jnp.float32).astype(jnp.bfloat16)
    context = context.reshape(n_tok, num_heads * head_dim)
    attn_out = jnp.dot(context, wo_flat, preferred_element_type=jnp.float32)
    hidden = (x_wide + attn_out).astype(jnp.bfloat16)
    inv_two, array_b8 = rms_parts(hidden.astype(jnp.float32))
    gain_two = mlp_gain.astype(jnp.float32)
    normed_mlp = (array_b8 * gain_two).astype(jnp.bfloat16)
    gate_pre = jnp.dot(normed_mlp, w_gate, preferred_element_type=jnp.float32)
    up_pre = jnp.dot(normed_mlp, w_up, preferred_element_type=jnp.float32)
    gate_sig = jax.nn.sigmoid(gate_pre)
    gate_act = gate_pre * gate_sig
    gated_act = (gate_act * up_pre).astype(jnp.bfloat16)
    g_down = jnp.einsum('nf,nd->fd', gated_act, dy_flat, preferred_element_type=jnp.float32)
    d_gated = jnp.einsum('nd,fd->nf', dy_flat, w_down, preferred_element_type=jnp.float32)
    d_up = (d_gated * gate_act).astype(jnp.bfloat16)
    d_gate = (d_gated * up_pre * gate_sig * (1.0 + gate_pre * (1.0 - gate_sig))).astype(jnp.bfloat16)
    g_gate = jnp.einsum('nd,nf->df', normed_mlp, d_gate, preferred_element_type=jnp.float32)
    g_up = jnp.einsum('nd,nf->df', normed_mlp, d_up, preferred_element_type=jnp.float32)
    d_normed_mlp = (jnp.einsum('nf,df->nd', d_gate, w_gate, preferred_element_type=jnp.float32)
                    + jnp.einsum('nf,df->nd', d_up, w_up, preferred_element_type=jnp.float32))
    g_mlp_gain = jnp.sum(d_normed_mlp * array_b8, axis=0)
    d_hidden = rms_back(d_normed_mlp, gain_two, inv_two, array_b8) + dy_flat.astype(jnp.float32)
    d_hidden_low = d_hidden.astype(jnp.bfloat16)
    g_out = jnp.einsum('nc,nd->cd', context, d_hidden_low, preferred_element_type=jnp.float32)
    d_context = jnp.einsum('nd,cd->nc', d_hidden_low, wo_flat, preferred_element_type=jnp.float32).astype(jnp.bfloat16)
    d_context = d_context.reshape(num_seqs, seq_len, kv_heads, group_size, head_dim)
    d_probs = jnp.einsum('bqkgd,bskd->bkgqs', d_context, v_heads, preferred_element_type=jnp.float32)
    g_values = jnp.einsum('bkgqs,bqkgd->bskd', probs_low, d_context, preferred_element_type=jnp.float32)
    d_scores = (attn_probs * (d_probs - jnp.sum(d_probs * attn_probs, axis=-1, keepdims=True)) * score_scale).astype(jnp.bfloat16)
    d_q_rot = jnp.einsum('bkgqs,bskd->bqkgd', d_scores, k_rot, preferred_element_type=jnp.float32).reshape(num_seqs, seq_len, num_heads, head_dim)
    d_k_rot = jnp.einsum('bkgqs,bqkgd->bskd', d_scores, q_rot, preferred_element_type=jnp.float32)
    d_q_pre = rope_back(d_q_rot, cos_full, sin_full).astype(jnp.bfloat16).reshape(n_tok, num_heads * head_dim)
    d_k_pre = rope_back(d_k_rot, cos_full, sin_full).astype(jnp.bfloat16).reshape(n_tok, kv_heads * head_dim)
    d_v_pre = g_values.astype(jnp.bfloat16).reshape(n_tok, kv_heads * head_dim)
    g_query = jnp.einsum('nd,nc->dc', normed, d_q_pre, preferred_element_type=jnp.float32)
    g_key = jnp.einsum('nd,nc->dc', normed, d_k_pre, preferred_element_type=jnp.float32)
    g_value = jnp.einsum('nd,nc->dc', normed, d_v_pre, preferred_element_type=jnp.float32)
    d_normed = (jnp.einsum('nc,dc->nd', d_q_pre, wq_flat, preferred_element_type=jnp.float32)
                + jnp.einsum('nc,dc->nd', d_k_pre, wk_flat, preferred_element_type=jnp.float32)
                + jnp.einsum('nc,dc->nd', d_v_pre, wv_flat, preferred_element_type=jnp.float32))
    g_attn_gain = jnp.sum(d_normed * value_a8, axis=0)
    d_x = rms_back(d_normed, gain_one, inv_one, value_a8) + d_hidden
    grad_list = [g_attn_gain, g_query, g_key, g_value, g_out, g_mlp_gain, g_gate, g_up, g_down]
    return d_x.astype(jnp.bfloat16).reshape(num_seqs, seq_len, model_dim), grad_list


def windows(grad_list):
    tiles = [g.astype(jnp.bfloat16).reshape(2, 8, 128) if g.ndim == 1 else to_tiles(g.astype(jnp.bfloat16)) for g in grad_list]
    moves = []
    for dev in range(NDEV):
        for mat in range(len(MATS)):
            a, b = overlap(BASE[dev], BASE[dev] + WIN_R, mat)
            if b > a:
                moves.append((mat, a - OFFS[mat], 0, dev * WIN_R + a - BASE[dev], b - a))
    return move(moves, tiles, (NDEV * WIN_R,))[0].reshape(NDEV, WIN_R, 8, 128)


def assemble(slots, w_list):
    moves = []
    for dev in range(NDEV):
        for mat in range(len(MATS)):
            a, b = overlap(OWN[dev], OWN[dev + 1], mat)
            if b > a:
                moves.append((0, dev * WIN_A + a - OWN[dev], mat, a - OFFS[mat], b - a))
    tiles = move(moves, [slots.reshape(NDEV * WIN_A, 8, 128)], tuple(m[0] for m in MATS))
    out = []
    for mat, weight in enumerate(w_list):
        if weight.ndim == 1:
            out.append(tiles[mat].reshape(weight.shape))
        else:
            cols = MATS[mat][1] * 128
            out.append(from_tiles(tiles[mat], weight.size // cols, cols).reshape(weight.shape))
    return out


def reduce_scatter(grad_list):
    return scatter(windows(grad_list))


def adamw(grad, clip_scale, master, mean, var, first_row):
    clipped = grad * clip_scale
    new_mean = BETA_ONE * mean + (1.0 - BETA_ONE) * clipped
    new_var = BETA_TWO * var + (1.0 - BETA_TWO) * clipped * clipped
    mean_hat = new_mean / (1.0 - BETA_ONE ** STEP_COUNT)
    var_hat = new_var / (1.0 - BETA_TWO ** STEP_COUNT)
    row = first_row + lax.broadcasted_iota(jnp.int32, master.shape, 0)
    gain_two = OFFS[5] * 8
    is_gain = (row < 16) | ((row >= gain_two) & (row < gain_two + 16))
    decays = jnp.where(is_gain, 0.0, WEIGHT_DECAY)
    new_master = master - LEARN_RATE * (mean_hat / (jnp.sqrt(var_hat) + ADAM_EPS) + decays * master)
    return new_master, new_mean, new_var


def update(win, master, mean, var, tab_in, tab_out):
    me = lax.axis_index('dp')
    state = [s.reshape(ROWS, 128) for s in (master, mean, var)]
    edge = jnp.stack([s[:HALO] for s in state])
    edge = lax.ppermute(edge, 'dp', [(d, d - 1) for d in range(1, NDEV)])
    summed = unpermute(jnp.asarray(tab_in)[me], win)
    grad = summed[HALO:HALO + ROWS] * (1.0 / NDEV)
    grad_edge = summed[HALO + ROWS:2 * HALO + ROWS] * (1.0 / NDEV)
    grad_norm = jnp.sqrt(lax.psum(jnp.sum(grad * grad), 'dp'))
    clip_scale = jnp.minimum(1.0, 1.0 / (grad_norm + 1e-6))
    new_state = adamw(grad, clip_scale, *state, me * ROWS)
    edge_master = adamw(grad_edge, clip_scale, edge[0], edge[1], edge[2], (me + 1) * ROWS)[0]
    shard = permute(jnp.asarray(tab_out)[me], new_state[0], edge_master)
    return [s.reshape(-1) for s in new_state], grad_norm, shard


def solution(mesh):
    tab_in, tab_out = tables()

    def per_device(x_loc, dy_loc, pos_loc, attn_gain, w_query, w_key, w_value, w_out, mlp_gain, w_gate, w_up, w_down, master_loc, mean_loc, var_loc):
        w_list = (attn_gain, w_query, w_key, w_value, w_out, mlp_gain, w_gate, w_up, w_down)
        grad_x, grad_list = local_grads(x_loc, dy_loc, pos_loc, w_list)
        win = reduce_scatter(grad_list)
        new_state, grad_norm, shard = update(win, master_loc, mean_loc, var_loc, tab_in, tab_out)
        new_weights = assemble(gather(shard), w_list)
        return (grad_x,) + tuple(new_weights) + tuple(new_state) + (grad_norm,)

    in_specs = (P('dp'),) * 3 + (P(),) * 9 + (P('dp'),) * 3
    out_specs = (P('dp'),) + (P(),) * 9 + (P('dp'),) * 3 + (P(),)
    return jax.shard_map(per_device, mesh=mesh, in_specs=in_specs, out_specs=out_specs, check_vma=False)
```

```python
import functools
import jax
import jax.numpy as jnp
import numpy as np
from jax import lax
from jax.experimental import pallas as pl
from jax.experimental.pallas import tpu as pltpu
from jax.sharding import PartitionSpec as P

NORM_EPS = 1e-5
ROPE_BASE = 10000.0
LEARN_RATE = 2e-3
BETA_ONE = 0.9
BETA_TWO = 0.95
ADAM_EPS = 1e-8
WEIGHT_DECAY = 0.1
STEP_COUNT = 100

MATS = ((2, 1), (4096, 16), (512, 2), (512, 2), (4096, 16), (2, 1), (11264, 44), (11264, 44), (11264, 16))
SUB, LANES = 8, 128
F32 = jnp.float32
OFFS = tuple(int(o) for o in np.cumsum([0] + [m[0] for m in MATS]))
NDEV = 32
TILES = OFFS[-1]
ROWS = TILES * 8 // NDEV
HALO = 352
WIN_R = 1408
WIN_A = 1376
S_ROWS = 11464
X_ROWS = 11112


def group_of(row):
    tile = row // 8
    mat = max(m for m in range(len(MATS)) if OFFS[m] <= tile)
    per = MATS[mat][1]
    return OFFS[mat] + (tile - OFFS[mat]) // per * per, per


def plan():
    lo, hi, own = [], [], []
    for dev in range(NDEV):
        start, per = group_of(ROWS * dev)
        last, last_per = group_of(ROWS * (dev + 1) - 1)
        lo.append(start)
        hi.append(last + last_per)
        own.append(start if start * SUB == ROWS * dev else start + per)
    own.append(TILES)
    return lo, hi, own


LO, HI, OWN = plan()
BASE = [min(a, TILES - WIN_R) for a in LO]


def overlap(a, b, mat):
    return max(a, OFFS[mat]), min(b, OFFS[mat + 1])


def tables():
    rows_in, rows_out = [], []
    for dev in range(NDEV):
        r_in, r_out = [], []
        for mat, (_, per) in enumerate(MATS):
            a, b = overlap(LO[dev], HI[dev], mat)
            n = max(0, b - a) // per
            r_in += [a - BASE[dev], SUB * a - ROWS * dev + HALO, n] if n else [0, 0, 0]
            a, b = overlap(OWN[dev], OWN[dev + 1], mat)
            n = max(0, b - a) // per
            r_out += [a - OWN[dev], SUB * a - ROWS * dev, n] if n else [0, 0, 0]
        rows_in.append(r_in)
        rows_out.append(r_out)
    return np.array(rows_in, np.int32), np.array(rows_out, np.int32)


def to_tiles(mat2d):
    rows, cols = mat2d.shape
    return mat2d.reshape(rows // SUB, SUB, cols // LANES, LANES).transpose(0, 2, 1, 3).reshape(-1, SUB, LANES)


def from_tiles(tiles, rows, cols):
    return tiles.reshape(rows // SUB, cols // LANES, SUB, LANES).transpose(0, 2, 1, 3).reshape(rows, cols)


def unpermute_kernel(tab, x_ref, o_ref):
    o_ref[0:HALO, :] = jnp.zeros((HALO, LANES), F32)
    o_ref[S_ROWS - HALO - 24:S_ROWS, :] = jnp.zeros((HALO + 24, LANES), F32)
    for mat, (_, per) in enumerate(MATS):
        t0, r0 = tab[3 * mat], tab[3 * mat + 1]

        def body(g, carry, per=per, t0=t0, r0=r0):
            for j in range(per):
                o_ref[pl.ds(r0 + g * (SUB * per) + j, SUB, stride=per), :] = x_ref[t0 + g * per + j].astype(F32)
            return carry

        lax.fori_loop(0, tab[3 * mat + 2], body, 0)


def unpermute(tab, win):
    return pl.pallas_call(
        unpermute_kernel,
        out_shape=jax.ShapeDtypeStruct((S_ROWS, LANES), F32),
        grid_spec=pltpu.PrefetchScalarGridSpec(
            num_scalar_prefetch=1, grid=(1,),
            in_specs=[pl.BlockSpec((WIN_R, SUB, LANES), lambda i, t: (0, 0, 0))],
            out_specs=pl.BlockSpec((S_ROWS, LANES), lambda i, t: (0, 0))),
        compiler_params=pltpu.CompilerParams(vmem_limit_bytes=40 << 20),
        cost_estimate=pl.CostEstimate(flops=4000000, bytes_accessed=9000000, transcendentals=0),
    )(tab, win)


def permute_kernel(tab, x_ref, h_ref, o_ref, s_ref):
    def fill(k, carry):
        at = pl.ds(pl.multiple_of(k * 64, 64), 64)
        s_ref[at, :] = x_ref[at, :]
        return carry

    lax.fori_loop(0, ROWS // 64, fill, 0)
    s_ref[ROWS // 64 * 64:ROWS, :] = x_ref[ROWS // 64 * 64:ROWS, :]
    s_ref[ROWS:ROWS + HALO, :] = h_ref[...]
    for mat, (_, per) in enumerate(MATS):
        t0, r0 = tab[3 * mat], tab[3 * mat + 1]

        def body(g, carry, per=per, t0=t0, r0=r0):
            for j in range(per):
                o_ref[t0 + g * per + j] = s_ref[pl.ds(r0 + g * (SUB * per) + j, SUB, stride=per), :].astype(jnp.bfloat16)
            return carry

        lax.fori_loop(0, tab[3 * mat + 2], body, 0)


def permute(tab, rows, halo):
    return pl.pallas_call(
        permute_kernel,
        out_shape=jax.ShapeDtypeStruct((WIN_A, SUB, LANES), jnp.bfloat16),
        grid_spec=pltpu.PrefetchScalarGridSpec(
            num_scalar_prefetch=1, grid=(1,),
            in_specs=[pl.BlockSpec((ROWS, LANES), lambda i, t: (0, 0)), pl.BlockSpec((HALO, LANES), lambda i, t: (0, 0))],
            out_specs=pl.BlockSpec((WIN_A, SUB, LANES), lambda i, t: (0, 0, 0)),
            scratch_shapes=[pltpu.VMEM((X_ROWS, LANES), F32)]),
        compiler_params=pltpu.CompilerParams(vmem_limit_bytes=40 << 20),
        cost_estimate=pl.CostEstimate(flops=4000000, bytes_accessed=9000000, transcendentals=0),
    )(tab, rows, halo)


SMALL = 152
ONE, TWO, SMALL_ONE, SMALL_TWO, SMALLS = range(5)


def parts_of(total):
    big = total // 2 - SMALL
    return (0, big), (big, big), (2 * big, SMALL), (2 * big + SMALL, SMALL), (2 * big, 2 * SMALL)


class Place:
    def __init__(self):
        me = lax.axis_index('dp')
        self.me = me
        self.core, self.xx, self.yy, self.zz = me % 2, (me // 2) % 2, (me // 4) % 2, me // 8
        self.mate, self.xn = self.at(self.zz, 0, 0, 1), self.at(self.zz, 0, 1, 0)
        self.yn, self.diag = self.at(self.zz, 1, 0, 0), self.at(self.zz, 1, 1, 0)
        self.up, self.down = self.at(self.zz + 1, 0, 0, 0), self.at(self.zz - 1, 0, 0, 0)
        self.has_up, self.has_down = self.zz < 3, self.zz > 0

    def at(self, z, dy, dx, dc):
        y, x, c = (1 - a if d else a for a, d in ((self.yy, dy), (self.xx, dx), (self.core, dc)))
        return ((z * 2 + y) * 2 + x) * 2 + c

    def greet(self):
        barrier = pltpu.get_barrier_semaphore()
        for cond, target in ((None, self.xn), (None, self.yn), (None, self.mate), (self.has_up, self.up), (self.has_down, self.down)):
            guarded(cond, lambda target=target: pl.semaphore_signal(
                barrier, device_id=(target,), device_id_type=pl.DeviceIdType.MESH))
        pl.semaphore_wait(barrier, 3 + self.has_up.astype(jnp.int32) + self.has_down.astype(jnp.int32))


def guarded(cond, body):
    if cond is None:
        body()
    else:
        pl.when(cond)(body)


def both(a, b):
    return b if a is None else a if b is None else jnp.logical_and(a, b)


def remote(src, dst, send, recv, target):
    return pltpu.make_async_remote_copy(src_ref=src, dst_ref=dst, send_sem=send, recv_sem=recv,
                                        device_id=(target,), device_id_type=pl.DeviceIdType.MESH)


PLANE = HERE, BY_X, BY_Y, BY_XY = (0, 0), (0, 1), (1, 0), (1, 1)


def gather_kernel(x_ref, out_ref, own_sem, send_sem, recv_sem):
    p = Place()
    p.greet()
    parts = parts_of(WIN_A)
    sent = []

    def view(slot, part, own=False):
        at = pl.ds(*parts[part])
        return x_ref.at[at] if own else out_ref.at[slot, at]

    def send(slot, part, target, cond=None, onward=None, own=False):
        desc = remote(view(slot, part, own), view(slot, part), send_sem.at[len(sent)], recv_sem.at[slot, part], target)
        sent.append((part, cond, onward))
        guarded(onward, desc.start)

    def arrived(slot, part):
        remote(view(slot, part), view(slot, part), send_sem.at[0], recv_sem.at[slot, part], p.mate).wait_recv()

    own_copy = pltpu.make_async_copy(x_ref, out_ref.at[p.me], own_sem)
    own_copy.start()
    send(p.me, SMALL_ONE, p.xn, own=True)
    send(p.me, SMALL_TWO, p.yn, own=True)
    for part in (ONE, TWO):
        send(p.me, part, p.up, None, p.has_up, True)
        send(p.me, part, p.down, None, p.has_down, True)
        send(p.me, part, p.xn, own=True)
        send(p.me, part, p.yn, own=True)
    send(p.me, SMALL_ONE, p.yn, own=True)
    send(p.me, SMALL_TWO, p.xn, own=True)
    for part in (ONE, TWO, SMALLS):
        send(p.me, part, p.mate, own=True)
    arrived(p.xn, SMALL_ONE)
    send(p.xn, SMALL_ONE, p.yn)
    arrived(p.yn, SMALL_TWO)
    send(p.yn, SMALL_TWO, p.xn)

    def steps(step):
        if step == 0:
            return [(None, p.zz, None, None)]
        return [(p.zz >= step, p.zz - step, p.up, p.has_up), (p.zz + step <= 3, p.zz + step, p.down, p.has_down)]

    def column(step):
        for cond, z, to, onward in steps(step):
            def body():
                slot = p.at(z, *HERE, 0)
                for part in (ONE, TWO):
                    arrived(slot, part)
                    send(slot, part, to, cond, onward)
                    for target in (p.xn, p.yn, p.mate):
                        send(slot, part, target, cond)
            guarded(cond, body)

    def beside(step):
        for cond, z, _, _ in steps(step):
            def body():
                for part in (ONE, TWO):
                    for dy, dx in (BY_X, BY_Y):
                        slot = p.at(z, dy, dx, 0)
                        arrived(slot, part)
                        if dy == part:
                            send(slot, part, p.xn if dy else p.yn, cond)
                        send(slot, part, p.mate, cond)
            guarded(cond, body)

    def across(step):
        for cond, z, _, _ in steps(step):
            def body():
                slot = p.at(z, *BY_XY, 0)
                for part in (ONE, TWO):
                    arrived(slot, part)
                    send(slot, part, p.mate, cond)
            guarded(cond, body)

    def plane():
        for dy, dx in PLANE:
            slot = p.at(p.zz, dy, dx, 0)
            own = dy + dx == 0
            if not own:
                if dy:
                    arrived(slot, SMALL_ONE)
                if dx:
                    arrived(slot, SMALL_TWO)
                send(slot, SMALLS, p.mate)
            send(slot, SMALLS, p.up, None, p.has_up, own)
            send(slot, SMALLS, p.down, None, p.has_down, own)

    def planes(step):
        for cond, z, to, onward in steps(step):
            def body():
                for dy, dx in PLANE:
                    slot = p.at(z, dy, dx, 0)
                    arrived(slot, SMALLS)
                    send(slot, SMALLS, to, cond, onward)
                    send(slot, SMALLS, p.mate, cond)
            guarded(cond, body)

    column(1)
    beside(0)
    column(2)
    plane()
    beside(1)
    across(0)
    column(3)
    beside(2)
    across(1)
    planes(1)
    beside(3)
    across(2)
    planes(2)
    across(3)
    planes(3)

    def drain(k, carry):
        for part in (ONE, TWO, SMALLS):
            arrived(2 * k + 1 - p.core, part)
        return carry

    lax.fori_loop(0, NDEV // 2, drain, 0)
    for k, (part, cond, onward) in enumerate(sent):
        done = remote(view(p.me, part), view(p.me, part), send_sem.at[k], recv_sem.at[p.me, part], p.mate).wait_send
        guarded(both(cond, onward), done)
    own_copy.wait()


def gather(shard):
    dma = pltpu.SemaphoreType.DMA
    return pl.pallas_call(
        gather_kernel,
        out_shape=jax.ShapeDtypeStruct((NDEV, WIN_A, SUB, LANES), jnp.bfloat16),
        in_specs=[pl.BlockSpec(memory_space=pltpu.VMEM)],
        out_specs=pl.BlockSpec(memory_space=pl.ANY),
        scratch_shapes=[dma, dma((200,)), dma((NDEV, 5))],
        compiler_params=pltpu.CompilerParams(collective_id=1, has_side_effects=True, vmem_limit_bytes=16 << 20),
    )(shard)


PIECES = ((*BY_XY, ONE), (*BY_XY, TWO), (*BY_Y, ONE), (*BY_X, TWO), (*BY_X, ONE), (*BY_Y, TWO), (*HERE, ONE), (*HERE, TWO))


def scatter_kernel(src_ref, out_ref, land_mate, land_hop, land_z, acc, tmp, load_sem, tmp_sem, out_sem, send_sem, mate_sem, hop_sem, z_sem):
    p = Place()
    p.greet()
    parts = parts_of(WIN_R)
    sent = []

    low = jnp.minimum(p.zz, 3 - p.zz)
    order = []
    for far, near in ((3, 3), (2, 0), (1, 2)):
        at = jnp.where(low == 0, far, near)
        order.append(jnp.where(p.zz >= 2, 3 - at, at))
    order.append(p.zz)

    def here(k, dy, dx, part):
        return acc.at[k * 4 + dy * 2 + dx, pl.ds(*parts[part])]

    def fetch(k, dy, dx, part):
        at, i = pl.ds(*parts[part]), k * 4 + dy * 2 + dx
        own = pltpu.make_async_copy(src_ref.at[p.at(order[k], dy, dx, 0), at], here(k, dy, dx, part), load_sem.at[i, min(part, 2)])
        give = remote(src_ref.at[p.at(order[k], dy, dx, 1), at], land_mate.at[i, at], send_sem.at[i, min(part, 2)], mate_sem.at[i, min(part, 2)], p.mate)
        return own, give, land_mate.at[i, at]

    def add(k, dy, dx, part, landed):
        start, count = parts[part]
        copy = pltpu.make_async_copy(landed, tmp.at[pl.ds(0, count)], tmp_sem)
        copy.start()
        copy.wait()
        i = k * 4 + dy * 2 + dx

        def body(t, carry):
            at, to = pl.ds(t * SUB, SUB), pl.ds(start + t * SUB, SUB)
            acc[i, to] = (acc[i, to].astype(F32) + tmp[at].astype(F32)).astype(jnp.bfloat16)
            return carry

        lax.fori_loop(0, count // SUB, body, 0)

    def begin(k, pieces):
        for piece in pieces:
            own, give, _ = fetch(k, *piece)
            give.start()
            own.start()

    def join(k, piece):
        own, give, landed = fetch(k, *piece)
        own.wait()
        give.wait_recv()
        add(k, *piece, landed)

    def hop(k, dy, dx, part, second):
        by_y = (part in (ONE, SMALL_ONE)) != second
        to_dy, to_dx = (0, dx) if by_y else (dy, 0)
        n = to_dy + to_dx + 2 * second
        dst = land_hop.at[k, n, pl.ds(*parts[part])]
        desc = remote(here(k, dy, dx, part), dst, send_sem.at[16 + k * 3 + n, part], hop_sem.at[k, n, part], p.yn if by_y else p.xn)
        return desc, dst, (16 + k * 3 + n, part)

    def leave(k, dy, dx, part, second=False):
        desc, _, key = hop(k, dy, dx, part, second)
        sent.append((key, part))
        desc.start()

    def enter(k, dy, dx, part, second=False):
        by_y = (part in (ONE, SMALL_ONE)) != second
        frm = (1, dx) if by_y else (dy, 1)
        desc, landed, _ = hop(k, *frm, part, second)
        desc.wait_recv()
        add(k, dy, dx, part, landed)

    def along(k, dy, dx, part, way):
        n = dy * 2 + dx
        at = pl.ds(*parts[part])
        key = (28 + k * 4 + n, min(part, 2))
        return remote(here(k, dy, dx, part), land_z.at[way, order[k], n, at], send_sem.at[key], z_sem.at[way, order[k], n, min(part, 2)],
                      p.down if way else p.up), land_z.at[way, order[k], n, at], key

    def collect(k, dy, dx, part):
        for way, cond in ((0, (order[k] >= p.zz) & p.has_down), (1, (order[k] <= p.zz) & p.has_up)):
            @pl.when(cond)
            def _():
                desc, landed, _ = along(k, dy, dx, part, way)
                desc.wait_recv()
                add(k, dy, dx, part, landed)

    def pass_on(k, dy, dx, part):
        for way, cond in ((0, order[k] > p.zz), (1, order[k] < p.zz)):
            @pl.when(cond)
            def _():
                along(k, dy, dx, part, way)[0].start()

    smalls = [(dy, dx, SMALLS) for dy, dx in PLANE]
    begin(0, smalls)
    begin(0, PIECES)
    begin(1, smalls)
    begin(2, smalls)
    begin(1, PIECES)
    begin(2, PIECES)
    begin(3, smalls)
    begin(3, PIECES)

    is_end = low == 0

    def small(k):
        for piece in smalls:
            join(k, piece)
        if k < 3:
            for piece in smalls:
                sent.append((along(k, *piece, 0)[2], SMALLS))
            pl.when(is_end)(lambda: [pass_on(k, *piece) for piece in smalls] and None)

    def chain(k):
        @pl.when(jnp.logical_not(is_end))
        def _():
            for piece in smalls:
                collect(k, *piece)
                pass_on(k, *piece)

    def prepare(k):
        for piece in PIECES:
            join(k, piece)
            if piece[piece[2]] == 1:
                leave(k, *piece)

    def second(k):
        for piece in ((*BY_X, ONE), (*BY_Y, TWO)):
            enter(k, *piece)
            leave(k, *piece, True)

    def final(k):
        for part in (ONE, TWO):
            enter(k, *HERE, part)
        for part in (ONE, TWO):
            enter(k, *HERE, part, True)
            collect(k, *HERE, part)
            if k < 3:
                sent.append((along(k, *HERE, part, 0)[2], part))
                pass_on(k, *HERE, part)

    small(0)
    prepare(0)
    small(1)
    small(2)
    prepare(1)
    chain(0)
    small(3)
    second(0)
    prepare(2)
    chain(1)
    second(1)
    chain(2)
    prepare(3)
    for piece in smalls:
        collect(3, *piece)
    for dy, dx, part in ((*BY_XY, SMALL_ONE), (*BY_XY, SMALL_TWO), (*BY_Y, SMALL_ONE), (*BY_X, SMALL_TWO)):
        leave(3, dy, dx, part)
    final(0)
    for piece in ((*BY_X, SMALL_ONE), (*BY_Y, SMALL_TWO)):
        enter(3, *piece)
        leave(3, *piece, True)
    second(2)
    final(1)
    second(3)
    for part in (SMALL_ONE, SMALL_TWO):
        enter(3, *HERE, part)
        enter(3, *HERE, part, True)
    final(2)
    final(3)
    out = pltpu.make_async_copy(acc.at[12], out_ref, out_sem)
    out.start()
    for k in range(4):
        for piece in PIECES + tuple(smalls):
            fetch(k, *piece)[1].wait_send()
    for key, part in sent:
        src = here(0, *HERE, part)
        remote(src, src, send_sem.at[key], z_sem.at[0, 0, 0, 0], p.mate).wait_send()
    out.wait()


def scatter(slots):
    def lands(*lead):
        return jax.ShapeDtypeStruct(lead + (WIN_R, SUB, LANES), jnp.bfloat16)

    any_spec = pl.BlockSpec(memory_space=pl.ANY)
    dma = pltpu.SemaphoreType.DMA
    return pl.pallas_call(
        scatter_kernel,
        out_shape=(lands(), lands(16), lands(4, 3), lands(2, 4, 4)),
        in_specs=[any_spec],
        out_specs=(any_spec,) * 4,
        scratch_shapes=[pltpu.VMEM((16, WIN_R, SUB, LANES), jnp.bfloat16), pltpu.VMEM((WIN_R // 2, SUB, LANES), jnp.bfloat16),
                        dma((16, 3)), dma, dma, dma((44, 4)), dma((16, 3)), dma((4, 3, 4)), dma((2, 4, 4, 3))],
        compiler_params=pltpu.CompilerParams(collective_id=2, has_side_effects=True, vmem_limit_bytes=56 << 20),
    )(slots)[0]


BUFS = 6


def move_kernel(moves, n_in, n_out, *refs):
    ins, outs = refs[:n_in], refs[n_in:n_in + n_out]
    buf, in_sem, out_sem = refs[n_in + n_out:]

    def read(n):
        src, a, _, _, count = moves[n]
        return pltpu.make_async_copy(ins[src].at[pl.ds(a, count)], buf.at[n % BUFS, pl.ds(0, count)], in_sem.at[n % BUFS])

    def write(n):
        _, _, dst, b, count = moves[n]
        return pltpu.make_async_copy(buf.at[n % BUFS, pl.ds(0, count)], outs[dst].at[pl.ds(b, count)], out_sem.at[n % BUFS])

    ahead = BUFS // 2
    for n in range(len(moves) + ahead):
        if n < len(moves):
            if n >= BUFS:
                write(n - BUFS).wait()
            read(n).start()
        if n >= ahead:
            read(n - ahead).wait()
            write(n - ahead).start()
    for n in range(max(0, len(moves) - BUFS), len(moves)):
        write(n).wait()


def move(moves, arrays, out_tiles):
    moves = tuple(m[:1] + (m[1] + c,) + m[2:3] + (m[3] + c, min(BLOCK, m[4] - c)) for m in moves for c in range(0, m[4], BLOCK))
    return pl.pallas_call(
        functools.partial(move_kernel, moves, len(arrays), len(out_tiles)),
        out_shape=tuple(jax.ShapeDtypeStruct((n, SUB, LANES), jnp.bfloat16) for n in out_tiles),
        in_specs=[pl.BlockSpec(memory_space=pl.ANY)] * len(arrays),
        out_specs=(pl.BlockSpec(memory_space=pl.ANY),) * len(out_tiles),
        scratch_shapes=[pltpu.VMEM((BUFS, BLOCK, SUB, LANES), jnp.bfloat16), pltpu.SemaphoreType.DMA((BUFS,)),
                        pltpu.SemaphoreType.DMA((BUFS,))],
        compiler_params=pltpu.CompilerParams(vmem_limit_bytes=20 << 20),
        cost_estimate=pl.CostEstimate(flops=100000000, bytes_accessed=176000000, transcendentals=0),
    )(*arrays)


BLOCK = 704


def norm_kernel(part_ref, out_ref, held, land, send_sem, recv_sem):
    me = lax.axis_index('dp')
    peers = [me + bit * (1 - 2 * ((me // bit) % 2)) for bit in (1, 2, 4, 8, 16)]
    barrier = pltpu.get_barrier_semaphore()
    for peer in peers:
        pl.semaphore_signal(barrier, inc=1, device_id=(peer,), device_id_type=pl.DeviceIdType.MESH)
    pl.semaphore_wait(barrier, 5)
    held[0] = part_ref[...]
    for n, peer in enumerate(peers):
        copy = pltpu.make_async_remote_copy(
            src_ref=held.at[n], dst_ref=land.at[n], send_sem=send_sem.at[n], recv_sem=recv_sem.at[n],
            device_id=(peer,), device_id_type=pl.DeviceIdType.MESH)
        copy.start()
        copy.wait()
        if n < 4:
            held[n + 1] = held[n] + land[n]
        else:
            out_ref[...] = held[n] + land[n]


def sum_over_devices(part):
    vmem = pl.BlockSpec(memory_space=pltpu.VMEM)
    rounds = pltpu.VMEM((5, SUB, LANES), F32)
    total = pl.pallas_call(
        norm_kernel,
        out_shape=jax.ShapeDtypeStruct((SUB, LANES), F32),
        in_specs=[vmem], out_specs=vmem,
        scratch_shapes=[rounds, rounds] + [pltpu.SemaphoreType.DMA((5,))] * 2,
        compiler_params=pltpu.CompilerParams(collective_id=3, has_side_effects=True, vmem_limit_bytes=4 << 20),
    )(jnp.full((SUB, LANES), part, F32))
    return total[0, 0]


def turn_kernel(x_ref, o_ref):
    rows = x_ref.shape[0] * 8
    o_ref[...] = x_ref[...].astype(F32).reshape(rows, LANES).T.astype(jnp.bfloat16)


def turned(tiles, rows, cols):
    return pl.pallas_call(
        turn_kernel,
        out_shape=jax.ShapeDtypeStruct((cols, rows), jnp.bfloat16),
        grid=(cols // LANES, rows // 1024),
        in_specs=[pl.BlockSpec((LANES, None, SUB, LANES), lambda j, i: (i, j, 0, 0))],
        out_specs=pl.BlockSpec((LANES, 1024), lambda j, i: (j, i)),
        cost_estimate=pl.CostEstimate(flops=rows * cols, bytes_accessed=4 * rows * cols, transcendentals=0),
    )(tiles.reshape(rows // SUB, cols // LANES, SUB, LANES))


def rope_tables(positions, head_dim):
    half_dim = head_dim // 2
    inv_freq = ROPE_BASE ** (-2.0 * jnp.arange(half_dim, dtype=F32) / head_dim)
    angles = positions.astype(F32)[:, :, None] * inv_freq
    cos_full = jnp.concatenate([jnp.cos(angles), jnp.cos(angles)], axis=-1)[:, :, None, :]
    sin_full = jnp.concatenate([jnp.sin(angles), jnp.sin(angles)], axis=-1)[:, :, None, :]
    return cos_full, sin_full


def rope_apply(values, cos_full, sin_full):
    half_dim = values.shape[-1] // 2
    rotated = jnp.concatenate([-values[..., half_dim:], values[..., :half_dim]], axis=-1)
    return values * cos_full + rotated * sin_full


def rope_back(grad_rot, cos_full, sin_full):
    half_dim = grad_rot.shape[-1] // 2
    scaled = grad_rot * sin_full
    return grad_rot * cos_full + jnp.concatenate([scaled[..., half_dim:], -scaled[..., :half_dim]], axis=-1)


def rms_parts(values):
    inv_rms = lax.rsqrt(jnp.mean(values * values, axis=-1, keepdims=True) + NORM_EPS)
    return inv_rms, values * inv_rms


def rms_back(d_normed, gain_wide, inv_rms, x_hat):
    d_hat = d_normed * gain_wide
    return inv_rms * (d_hat - x_hat * jnp.mean(d_hat * x_hat, axis=-1, keepdims=True))


def local_grads(x_loc, dy_loc, pos_loc, w_list):
    attn_gain, w_query, w_key, w_value, w_out, mlp_gain, w_gate, w_up, w_down = w_list
    num_seqs, seq_len, model_dim = x_loc.shape
    num_heads, head_dim = w_query.shape[1], w_query.shape[2]
    kv_heads = w_key.shape[1]
    group_size = num_heads // kv_heads
    n_tok = num_seqs * seq_len
    wq_flat = w_query.reshape(model_dim, num_heads * head_dim)
    wk_flat = w_key.reshape(model_dim, kv_heads * head_dim)
    wv_flat = w_value.reshape(model_dim, kv_heads * head_dim)
    wo_flat = w_out.reshape(num_heads * head_dim, model_dim)
    dy_flat = dy_loc.reshape(n_tok, model_dim)
    x_wide = x_loc.reshape(n_tok, model_dim).astype(F32)
    inv_one, value_a8 = rms_parts(x_wide)
    gain_one = attn_gain.astype(F32)
    normed = (value_a8 * gain_one).astype(jnp.bfloat16)
    q_pre = jnp.dot(normed, wq_flat, preferred_element_type=F32).reshape(num_seqs, seq_len, num_heads, head_dim)
    k_pre = jnp.dot(normed, wk_flat, preferred_element_type=F32).reshape(num_seqs, seq_len, kv_heads, head_dim)
    v_heads = jnp.dot(normed, wv_flat, preferred_element_type=F32).astype(jnp.bfloat16).reshape(num_seqs, seq_len, kv_heads, head_dim)
    cos_full, sin_full = rope_tables(pos_loc, head_dim)
    q_rot = rope_apply(q_pre, cos_full, sin_full).astype(jnp.bfloat16).reshape(num_seqs, seq_len, kv_heads, group_size, head_dim)
    k_rot = rope_apply(k_pre, cos_full, sin_full).astype(jnp.bfloat16)
    score_scale = head_dim ** -0.5
    scores = jnp.einsum('bqkgd,bskd->bkgqs', q_rot, k_rot, preferred_element_type=F32) * score_scale
    causal = lax.iota(jnp.int32, seq_len)[:, None] >= lax.iota(jnp.int32, seq_len)[None, :]
    attn_probs = jax.nn.softmax(jnp.where(causal, scores, -1e30), axis=-1)
    probs_low = attn_probs.astype(jnp.bfloat16)
    context = jnp.einsum('bkgqs,bskd->bqkgd', probs_low, v_heads, preferred_element_type=F32).astype(jnp.bfloat16)
    context = context.reshape(n_tok, num_heads * head_dim)
    attn_out = jnp.dot(context, wo_flat, preferred_element_type=F32)
    hidden = (x_wide + attn_out).astype(jnp.bfloat16)
    inv_two, array_b8 = rms_parts(hidden.astype(F32))
    gain_two = mlp_gain.astype(F32)
    normed_mlp = (array_b8 * gain_two).astype(jnp.bfloat16)
    gate_pre = jnp.dot(normed_mlp, w_gate, preferred_element_type=F32)
    up_pre = jnp.dot(normed_mlp, w_up, preferred_element_type=F32)
    gate_sig = jax.nn.sigmoid(gate_pre)
    gate_act = gate_pre * gate_sig
    gated_act = (gate_act * up_pre).astype(jnp.bfloat16)
    g_down = jnp.einsum('nf,nd->fd', gated_act, dy_flat, preferred_element_type=F32)
    d_gated = jnp.einsum('nd,fd->nf', dy_flat, w_down, preferred_element_type=F32)
    d_up = (d_gated * gate_act).astype(jnp.bfloat16)
    d_gate = (d_gated * up_pre * gate_sig * (1.0 + gate_pre * (1.0 - gate_sig))).astype(jnp.bfloat16)
    g_gate = jnp.einsum('nd,nf->df', normed_mlp, d_gate, preferred_element_type=F32)
    g_up = jnp.einsum('nd,nf->df', normed_mlp, d_up, preferred_element_type=F32)
    d_normed_mlp = (jnp.einsum('nf,df->nd', d_gate, w_gate, preferred_element_type=F32)
                    + jnp.einsum('nf,df->nd', d_up, w_up, preferred_element_type=F32))
    g_mlp_gain = jnp.sum(d_normed_mlp * array_b8, axis=0)
    d_hidden = rms_back(d_normed_mlp, gain_two, inv_two, array_b8) + dy_flat.astype(F32)
    d_hidden_low = d_hidden.astype(jnp.bfloat16)
    g_out = jnp.einsum('nc,nd->cd', context, d_hidden_low, preferred_element_type=F32)
    d_context = jnp.einsum('nd,cd->nc', d_hidden_low, wo_flat, preferred_element_type=F32).astype(jnp.bfloat16)
    d_context = d_context.reshape(num_seqs, seq_len, kv_heads, group_size, head_dim)
    d_probs = jnp.einsum('bqkgd,bskd->bkgqs', d_context, v_heads, preferred_element_type=F32)
    g_values = jnp.einsum('bkgqs,bqkgd->bskd', probs_low, d_context, preferred_element_type=F32)
    d_scores = (attn_probs * (d_probs - jnp.sum(d_probs * attn_probs, axis=-1, keepdims=True)) * score_scale).astype(jnp.bfloat16)
    d_q_rot = jnp.einsum('bkgqs,bskd->bqkgd', d_scores, k_rot, preferred_element_type=F32).reshape(num_seqs, seq_len, num_heads, head_dim)
    d_k_rot = jnp.einsum('bkgqs,bqkgd->bskd', d_scores, q_rot, preferred_element_type=F32)
    d_q_pre = rope_back(d_q_rot, cos_full, sin_full).astype(jnp.bfloat16).reshape(n_tok, num_heads * head_dim)
    d_k_pre = rope_back(d_k_rot, cos_full, sin_full).astype(jnp.bfloat16).reshape(n_tok, kv_heads * head_dim)
    d_v_pre = g_values.astype(jnp.bfloat16).reshape(n_tok, kv_heads * head_dim)
    g_query = jnp.einsum('nd,nc->dc', normed, d_q_pre, preferred_element_type=F32)
    g_key = jnp.einsum('nd,nc->dc', normed, d_k_pre, preferred_element_type=F32)
    g_value = jnp.einsum('nd,nc->dc', normed, d_v_pre, preferred_element_type=F32)
    d_normed = (jnp.einsum('nc,dc->nd', d_q_pre, wq_flat, preferred_element_type=F32)
                + jnp.einsum('nc,dc->nd', d_k_pre, wk_flat, preferred_element_type=F32)
                + jnp.einsum('nc,dc->nd', d_v_pre, wv_flat, preferred_element_type=F32))
    g_attn_gain = jnp.sum(d_normed * value_a8, axis=0)
    d_x = rms_back(d_normed, gain_one, inv_one, value_a8) + d_hidden
    grad_list = [g_attn_gain, g_query, g_key, g_value, g_out, g_mlp_gain, g_gate, g_up, g_down]
    return d_x.astype(jnp.bfloat16).reshape(num_seqs, seq_len, model_dim), grad_list


def windows(grad_list):
    tiles = [g.astype(jnp.bfloat16).reshape(2, SUB, LANES) if g.ndim == 1 else to_tiles(g.astype(jnp.bfloat16)) for g in grad_list]
    moves = []
    for dev in range(NDEV):
        for mat in range(len(MATS)):
            a, b = overlap(BASE[dev], BASE[dev] + WIN_R, mat)
            if b > a:
                moves.append((mat, a - OFFS[mat], 0, dev * WIN_R + a - BASE[dev], b - a))
    return move(moves, tiles, (NDEV * WIN_R,))[0].reshape(NDEV, WIN_R, SUB, LANES)


def assemble(slots, w_list):
    moves = []
    for dev in range(NDEV):
        for mat in range(len(MATS)):
            a, b = overlap(OWN[dev], OWN[dev + 1], mat)
            if b > a:
                moves.append((0, dev * WIN_A + a - OWN[dev], mat, a - OFFS[mat], b - a))
    tiles = move(moves, [slots.reshape(NDEV * WIN_A, SUB, LANES)], tuple(m[0] for m in MATS))
    out = []
    for mat, weight in enumerate(w_list):
        if weight.ndim == 1:
            out.append(tiles[mat].reshape(weight.shape))
        else:
            cols = MATS[mat][1] * LANES
            rows = weight.size // cols
            if mat in (1, 2, 3):
                flat = turned(tiles[mat], rows, cols)
                out.append(flat.reshape(weight.shape[1:] + weight.shape[:1]).transpose(2, 0, 1))
            else:
                out.append(from_tiles(tiles[mat], rows, cols).reshape(weight.shape))
    return out


def reduce_scatter(grad_list):
    return scatter(windows(grad_list))


def adamw(grad, clip_scale, master, mean, var, first_row):
    clipped = grad * clip_scale
    new_mean = BETA_ONE * mean + (1.0 - BETA_ONE) * clipped
    new_var = BETA_TWO * var + (1.0 - BETA_TWO) * clipped * clipped
    mean_hat = new_mean / (1.0 - BETA_ONE ** STEP_COUNT)
    var_hat = new_var / (1.0 - BETA_TWO ** STEP_COUNT)
    row = first_row + lax.broadcasted_iota(jnp.int32, master.shape, 0)
    gain_two = OFFS[5] * 8
    is_gain = (row < 16) | ((row >= gain_two) & (row < gain_two + 16))
    decays = jnp.where(is_gain, 0.0, WEIGHT_DECAY)
    new_master = master - LEARN_RATE * (mean_hat / (jnp.sqrt(var_hat) + ADAM_EPS) + decays * master)
    return new_master, new_mean, new_var


def update(win, master, mean, var, tab_in, tab_out):
    me = lax.axis_index('dp')
    state = [s.reshape(ROWS, LANES) for s in (master, mean, var)]
    edge = jnp.stack([s[:HALO] for s in state])
    edge = lax.ppermute(edge, 'dp', [(d, d - 1) for d in range(1, NDEV)])
    summed = unpermute(jnp.asarray(tab_in)[me], win)
    grad = summed[HALO:HALO + ROWS] * (1.0 / NDEV)
    grad_edge = summed[HALO + ROWS:2 * HALO + ROWS] * (1.0 / NDEV)
    grad_norm = jnp.sqrt(sum_over_devices(jnp.sum(grad * grad)))
    clip_scale = jnp.minimum(1.0, 1.0 / (grad_norm + 1e-6))
    new_state = adamw(grad, clip_scale, *state, me * ROWS)
    edge_master = adamw(grad_edge, clip_scale, edge[0], edge[1], edge[2], (me + 1) * ROWS)[0]
    shard = permute(jnp.asarray(tab_out)[me], new_state[0], edge_master)
    return [s.reshape(-1) for s in new_state], grad_norm, shard


def solution(mesh):
    tab_in, tab_out = tables()

    def per_device(x_loc, dy_loc, pos_loc, attn_gain, w_query, w_key, w_value, w_out, mlp_gain, w_gate, w_up, w_down, master_loc, mean_loc, var_loc):
        w_list = (attn_gain, w_query, w_key, w_value, w_out, mlp_gain, w_gate, w_up, w_down)
        grad_x, grad_list = local_grads(x_loc, dy_loc, pos_loc, w_list)
        win = reduce_scatter(grad_list)
        new_state, grad_norm, shard = update(win, master_loc, mean_loc, var_loc, tab_in, tab_out)
        new_weights = assemble(gather(shard), w_list)
        return (grad_x,) + tuple(new_weights) + tuple(new_state) + (grad_norm,)

    in_specs = (P('dp'),) * 3 + (P(),) * 9 + (P('dp'),) * 3
    out_specs = (P('dp'),) + (P(),) * 9 + (P('dp'),) * 3 + (P(),)
    return jax.shard_map(per_device, mesh=mesh, in_specs=in_specs, out_specs=out_specs, check_vma=False)
```

```python
import functools
import jax
import jax.numpy as jnp
import numpy as np
from jax import lax
from jax.experimental import pallas as pl
from jax.experimental.pallas import tpu as pltpu
from jax.sharding import PartitionSpec as P

NORM_EPS = 1e-5
ROPE_BASE = 10000.0
LEARN_RATE = 2e-3
BETA_ONE = 0.9
BETA_TWO = 0.95
ADAM_EPS = 1e-8
WEIGHT_DECAY = 0.1
STEP_COUNT = 100

MATS = ((2, 1), (4096, 16), (512, 2), (512, 2), (4096, 16), (2, 1), (11264, 44), (11264, 44), (11264, 16))
SUB, LANES = 8, 128
F32 = jnp.float32
OFFS = tuple(int(o) for o in np.cumsum([0] + [m[0] for m in MATS]))
NDEV = 32
TILES = OFFS[-1]
ROWS = TILES * 8 // NDEV
HALO = 352
WIN_R = 1408
WIN_A = 1376
S_ROWS = 11464
X_ROWS = 11112


def group_of(row):
    tile = row // 8
    mat = max(m for m in range(len(MATS)) if OFFS[m] <= tile)
    per = MATS[mat][1]
    return OFFS[mat] + (tile - OFFS[mat]) // per * per, per


def plan():
    lo, hi, own = [], [], []
    for dev in range(NDEV):
        start, per = group_of(ROWS * dev)
        last, last_per = group_of(ROWS * (dev + 1) - 1)
        lo.append(start)
        hi.append(last + last_per)
        own.append(start if start * SUB == ROWS * dev else start + per)
    own.append(TILES)
    return lo, hi, own


LO, HI, OWN = plan()
BASE = [min(a, TILES - WIN_R) for a in LO]


def overlap(a, b, mat):
    return max(a, OFFS[mat]), min(b, OFFS[mat + 1])


def tables():
    rows_in, rows_out = [], []
    for dev in range(NDEV):
        r_in, r_out = [], []
        for mat, (_, per) in enumerate(MATS):
            a, b = overlap(LO[dev], HI[dev], mat)
            n = max(0, b - a) // per
            r_in += [a - BASE[dev], SUB * a - ROWS * dev + HALO, n] if n else [0, 0, 0]
            a, b = overlap(OWN[dev], OWN[dev + 1], mat)
            n = max(0, b - a) // per
            r_out += [a - OWN[dev], SUB * a - ROWS * dev, n] if n else [0, 0, 0]
        rows_in.append(r_in)
        rows_out.append(r_out)
    return np.array(rows_in, np.int32), np.array(rows_out, np.int32)


def to_tiles(mat2d):
    rows, cols = mat2d.shape
    return mat2d.reshape(rows // SUB, SUB, cols // LANES, LANES).transpose(0, 2, 1, 3).reshape(-1, SUB, LANES)


def from_tiles(tiles, rows, cols):
    return tiles.reshape(rows // SUB, cols // LANES, SUB, LANES).transpose(0, 2, 1, 3).reshape(rows, cols)


def unpermute_kernel(tab, x_ref, o_ref):
    o_ref[0:HALO, :] = jnp.zeros((HALO, LANES), F32)
    o_ref[S_ROWS - HALO - 24:S_ROWS, :] = jnp.zeros((HALO + 24, LANES), F32)
    for mat, (_, per) in enumerate(MATS):
        t0, r0 = tab[3 * mat], tab[3 * mat + 1]

        def body(g, carry, per=per, t0=t0, r0=r0):
            for j in range(per):
                o_ref[pl.ds(r0 + g * (SUB * per) + j, SUB, stride=per), :] = x_ref[t0 + g * per + j].astype(F32)
            return carry

        lax.fori_loop(0, tab[3 * mat + 2], body, 0)


def unpermute(tab, win):
    return pl.pallas_call(
        unpermute_kernel,
        out_shape=jax.ShapeDtypeStruct((S_ROWS, LANES), F32),
        grid_spec=pltpu.PrefetchScalarGridSpec(
            num_scalar_prefetch=1, grid=(1,),
            in_specs=[pl.BlockSpec((WIN_R, SUB, LANES), lambda i, t: (0, 0, 0))],
            out_specs=pl.BlockSpec((S_ROWS, LANES), lambda i, t: (0, 0))),
        compiler_params=pltpu.CompilerParams(vmem_limit_bytes=40 << 20),
        cost_estimate=pl.CostEstimate(flops=4000000, bytes_accessed=9000000, transcendentals=0),
    )(tab, win)


def permute_kernel(tab, x_ref, h_ref, o_ref, s_ref):
    def fill(k, carry):
        at = pl.ds(pl.multiple_of(k * 64, 64), 64)
        s_ref[at, :] = x_ref[at, :]
        return carry

    lax.fori_loop(0, ROWS // 64, fill, 0)
    s_ref[ROWS // 64 * 64:ROWS, :] = x_ref[ROWS // 64 * 64:ROWS, :]
    s_ref[ROWS:ROWS + HALO, :] = h_ref[...]
    for mat, (_, per) in enumerate(MATS):
        t0, r0 = tab[3 * mat], tab[3 * mat + 1]

        def body(g, carry, per=per, t0=t0, r0=r0):
            for j in range(per):
                o_ref[t0 + g * per + j] = s_ref[pl.ds(r0 + g * (SUB * per) + j, SUB, stride=per), :].astype(jnp.bfloat16)
            return carry

        lax.fori_loop(0, tab[3 * mat + 2], body, 0)


def permute(tab, rows, halo):
    return pl.pallas_call(
        permute_kernel,
        out_shape=jax.ShapeDtypeStruct((WIN_A, SUB, LANES), jnp.bfloat16),
        grid_spec=pltpu.PrefetchScalarGridSpec(
            num_scalar_prefetch=1, grid=(1,),
            in_specs=[pl.BlockSpec((ROWS, LANES), lambda i, t: (0, 0)), pl.BlockSpec((HALO, LANES), lambda i, t: (0, 0))],
            out_specs=pl.BlockSpec((WIN_A, SUB, LANES), lambda i, t: (0, 0, 0)),
            scratch_shapes=[pltpu.VMEM((X_ROWS, LANES), F32)]),
        compiler_params=pltpu.CompilerParams(vmem_limit_bytes=40 << 20),
        cost_estimate=pl.CostEstimate(flops=4000000, bytes_accessed=9000000, transcendentals=0),
    )(tab, rows, halo)


SMALL = 152
ONE, TWO, SMALL_ONE, SMALL_TWO, SMALLS = range(5)


def parts_of(total):
    big = total // 2 - SMALL
    return (0, big), (big, big), (2 * big, SMALL), (2 * big + SMALL, SMALL), (2 * big, 2 * SMALL)


class Place:
    def __init__(self):
        me = lax.axis_index('dp')
        self.me = me
        self.core, self.xx, self.yy, self.zz = me % 2, (me // 2) % 2, (me // 4) % 2, me // 8
        self.mate, self.xn = self.at(self.zz, 0, 0, 1), self.at(self.zz, 0, 1, 0)
        self.yn, self.diag = self.at(self.zz, 1, 0, 0), self.at(self.zz, 1, 1, 0)
        self.up, self.down = self.at(self.zz + 1, 0, 0, 0), self.at(self.zz - 1, 0, 0, 0)
        self.has_up, self.has_down = self.zz < 3, self.zz > 0

    def at(self, z, dy, dx, dc):
        y, x, c = (1 - a if d else a for a, d in ((self.yy, dy), (self.xx, dx), (self.core, dc)))
        return ((z * 2 + y) * 2 + x) * 2 + c

    def greet(self):
        barrier = pltpu.get_barrier_semaphore()
        for cond, target in ((None, self.xn), (None, self.yn), (None, self.mate), (self.has_up, self.up), (self.has_down, self.down)):
            guarded(cond, lambda target=target: pl.semaphore_signal(
                barrier, device_id=(target,), device_id_type=pl.DeviceIdType.MESH))
        pl.semaphore_wait(barrier, 3 + self.has_up.astype(jnp.int32) + self.has_down.astype(jnp.int32))


def guarded(cond, body):
    if cond is None:
        body()
    else:
        pl.when(cond)(body)


def both(a, b):
    return b if a is None else a if b is None else jnp.logical_and(a, b)


def remote(src, dst, send, recv, target):
    return pltpu.make_async_remote_copy(src_ref=src, dst_ref=dst, send_sem=send, recv_sem=recv,
                                        device_id=(target,), device_id_type=pl.DeviceIdType.MESH)


PLANE = HERE, BY_X, BY_Y, BY_XY = (0, 0), (0, 1), (1, 0), (1, 1)


def gather_kernel(x_ref, out_ref, own_sem, send_sem, recv_sem):
    p = Place()
    p.greet()
    parts = parts_of(WIN_A)
    sent = []

    def view(slot, part, own=False):
        at = pl.ds(*parts[part])
        return x_ref.at[at] if own else out_ref.at[slot, at]

    def send(slot, part, target, cond=None, onward=None, own=False):
        desc = remote(view(slot, part, own), view(slot, part), send_sem.at[len(sent)], recv_sem.at[slot, part], target)
        sent.append((part, cond, onward))
        guarded(onward, desc.start)

    def arrived(slot, part):
        remote(view(slot, part), view(slot, part), send_sem.at[0], recv_sem.at[slot, part], p.mate).wait_recv()

    own_copy = pltpu.make_async_copy(x_ref, out_ref.at[p.me], own_sem)
    own_copy.start()
    send(p.me, SMALL_ONE, p.xn, own=True)
    send(p.me, SMALL_TWO, p.yn, own=True)
    for part in (ONE, TWO):
        send(p.me, part, p.up, None, p.has_up, True)
        send(p.me, part, p.down, None, p.has_down, True)
        send(p.me, part, p.xn, own=True)
        send(p.me, part, p.yn, own=True)
    send(p.me, SMALL_ONE, p.yn, own=True)
    send(p.me, SMALL_TWO, p.xn, own=True)
    for part in (ONE, TWO, SMALLS):
        send(p.me, part, p.mate, own=True)
    arrived(p.xn, SMALL_ONE)
    send(p.xn, SMALL_ONE, p.yn)
    arrived(p.yn, SMALL_TWO)
    send(p.yn, SMALL_TWO, p.xn)

    def steps(step):
        if step == 0:
            return [(None, p.zz, None, None)]
        return [(p.zz >= step, p.zz - step, p.up, p.has_up), (p.zz + step <= 3, p.zz + step, p.down, p.has_down)]

    def column(step):
        for cond, z, to, onward in steps(step):
            def body():
                slot = p.at(z, *HERE, 0)
                for part in (ONE, TWO):
                    arrived(slot, part)
                    send(slot, part, to, cond, onward)
                    for target in (p.xn, p.yn, p.mate):
                        send(slot, part, target, cond)
            guarded(cond, body)

    def beside(step):
        for cond, z, _, _ in steps(step):
            def body():
                for part in (ONE, TWO):
                    for dy, dx in (BY_X, BY_Y):
                        slot = p.at(z, dy, dx, 0)
                        arrived(slot, part)
                        if dy == part:
                            send(slot, part, p.xn if dy else p.yn, cond)
                        send(slot, part, p.mate, cond)
            guarded(cond, body)

    def across(step):
        for cond, z, _, _ in steps(step):
            def body():
                slot = p.at(z, *BY_XY, 0)
                for part in (ONE, TWO):
                    arrived(slot, part)
                    send(slot, part, p.mate, cond)
            guarded(cond, body)

    def plane():
        for dy, dx in PLANE:
            slot = p.at(p.zz, dy, dx, 0)
            own = dy + dx == 0
            if not own:
                if dy:
                    arrived(slot, SMALL_ONE)
                if dx:
                    arrived(slot, SMALL_TWO)
                send(slot, SMALLS, p.mate)
            send(slot, SMALLS, p.up, None, p.has_up, own)
            send(slot, SMALLS, p.down, None, p.has_down, own)

    def planes(step):
        for cond, z, to, onward in steps(step):
            def body():
                for dy, dx in PLANE:
                    slot = p.at(z, dy, dx, 0)
                    arrived(slot, SMALLS)
                    send(slot, SMALLS, to, cond, onward)
                    send(slot, SMALLS, p.mate, cond)
            guarded(cond, body)

    column(1)
    beside(0)
    column(2)
    plane()
    beside(1)
    across(0)
    column(3)
    planes(1)
    beside(2)
    planes(2)
    across(1)
    beside(3)
    across(2)
    planes(3)
    across(3)

    def drain(k, carry):
        for part in (ONE, TWO, SMALLS):
            arrived(2 * k + 1 - p.core, part)
        return carry

    lax.fori_loop(0, NDEV // 2, drain, 0)
    for k, (part, cond, onward) in enumerate(sent):
        done = remote(view(p.me, part), view(p.me, part), send_sem.at[k], recv_sem.at[p.me, part], p.mate).wait_send
        guarded(both(cond, onward), done)
    own_copy.wait()


def gather(shard):
    dma = pltpu.SemaphoreType.DMA
    return pl.pallas_call(
        gather_kernel,
        out_shape=jax.ShapeDtypeStruct((NDEV, WIN_A, SUB, LANES), jnp.bfloat16),
        in_specs=[pl.BlockSpec(memory_space=pltpu.VMEM)],
        out_specs=pl.BlockSpec(memory_space=pl.ANY),
        scratch_shapes=[dma, dma((200,)), dma((NDEV, 5))],
        compiler_params=pltpu.CompilerParams(collective_id=1, has_side_effects=True, vmem_limit_bytes=16 << 20),
    )(shard)


PIECES = ((*BY_XY, ONE), (*BY_XY, TWO), (*BY_Y, ONE), (*BY_X, TWO), (*BY_X, ONE), (*BY_Y, TWO), (*HERE, ONE), (*HERE, TWO))


def scatter_kernel(src_ref, out_ref, land_mate, land_hop, land_z, acc, tmp, load_sem, tmp_sem, out_sem, send_sem, mate_sem, hop_sem, z_sem):
    p = Place()
    p.greet()
    parts = parts_of(WIN_R)
    sent = []

    low = jnp.minimum(p.zz, 3 - p.zz)
    order = []
    for far, near in ((3, 3), (2, 0), (1, 2)):
        at = jnp.where(low == 0, far, near)
        order.append(jnp.where(p.zz >= 2, 3 - at, at))
    order.append(p.zz)

    def here(k, dy, dx, part):
        return acc.at[k * 4 + dy * 2 + dx, pl.ds(*parts[part])]

    def fetch(k, dy, dx, part):
        at, i = pl.ds(*parts[part]), k * 4 + dy * 2 + dx
        own = pltpu.make_async_copy(src_ref.at[p.at(order[k], dy, dx, 0), at], here(k, dy, dx, part), load_sem.at[i, min(part, 2)])
        give = remote(src_ref.at[p.at(order[k], dy, dx, 1), at], land_mate.at[i, at], send_sem.at[i, min(part, 2)], mate_sem.at[i, min(part, 2)], p.mate)
        return own, give, land_mate.at[i, at]

    def add(k, dy, dx, part, landed):
        start, count = parts[part]
        copy = pltpu.make_async_copy(landed, tmp.at[pl.ds(0, count)], tmp_sem)
        copy.start()
        copy.wait()
        i = k * 4 + dy * 2 + dx

        def body(t, carry):
            at, to = pl.ds(t * SUB, SUB), pl.ds(start + t * SUB, SUB)
            acc[i, to] = (acc[i, to].astype(F32) + tmp[at].astype(F32)).astype(jnp.bfloat16)
            return carry

        lax.fori_loop(0, count // SUB, body, 0)

    def begin(k, pieces):
        for piece in pieces:
            own, give, _ = fetch(k, *piece)
            give.start()
            own.start()

    def join(k, piece):
        own, give, landed = fetch(k, *piece)
        own.wait()
        give.wait_recv()
        add(k, *piece, landed)

    def hop(k, dy, dx, part, second):
        by_y = (part in (ONE, SMALL_ONE)) != second
        to_dy, to_dx = (0, dx) if by_y else (dy, 0)
        n = to_dy + to_dx + 2 * second
        dst = land_hop.at[k, n, pl.ds(*parts[part])]
        desc = remote(here(k, dy, dx, part), dst, send_sem.at[16 + k * 3 + n, part], hop_sem.at[k, n, part], p.yn if by_y else p.xn)
        return desc, dst, (16 + k * 3 + n, part)

    def leave(k, dy, dx, part, second=False):
        desc, _, key = hop(k, dy, dx, part, second)
        sent.append((key, part))
        desc.start()

    def enter(k, dy, dx, part, second=False):
        by_y = (part in (ONE, SMALL_ONE)) != second
        frm = (1, dx) if by_y else (dy, 1)
        desc, landed, _ = hop(k, *frm, part, second)
        desc.wait_recv()
        add(k, dy, dx, part, landed)

    def along(k, dy, dx, part, way):
        n = dy * 2 + dx
        at = pl.ds(*parts[part])
        key = (28 + k * 4 + n, min(part, 2))
        return remote(here(k, dy, dx, part), land_z.at[way, order[k], n, at], send_sem.at[key], z_sem.at[way, order[k], n, min(part, 2)],
                      p.down if way else p.up), land_z.at[way, order[k], n, at], key

    def collect(k, dy, dx, part):
        for way, cond in ((0, (order[k] >= p.zz) & p.has_down), (1, (order[k] <= p.zz) & p.has_up)):
            @pl.when(cond)
            def _():
                desc, landed, _ = along(k, dy, dx, part, way)
                desc.wait_recv()
                add(k, dy, dx, part, landed)

    def pass_on(k, dy, dx, part):
        for way, cond in ((0, order[k] > p.zz), (1, order[k] < p.zz)):
            @pl.when(cond)
            def _():
                along(k, dy, dx, part, way)[0].start()

    smalls = [(dy, dx, SMALLS) for dy, dx in PLANE]
    begin(0, smalls)
    begin(0, PIECES)
    begin(1, smalls)
    begin(2, smalls)
    begin(1, PIECES)
    begin(2, PIECES)
    begin(3, smalls)
    begin(3, PIECES)

    is_end = low == 0

    def small(k):
        for piece in smalls:
            join(k, piece)
        if k < 3:
            for piece in smalls:
                sent.append((along(k, *piece, 0)[2], SMALLS))
            pl.when(is_end)(lambda: [pass_on(k, *piece) for piece in smalls] and None)

    def chain(k):
        @pl.when(jnp.logical_not(is_end))
        def _():
            for piece in smalls:
                collect(k, *piece)
                pass_on(k, *piece)

    def prepare(k):
        for piece in PIECES:
            join(k, piece)
            if piece[piece[2]] == 1:
                leave(k, *piece)

    def second(k):
        for piece in ((*BY_X, ONE), (*BY_Y, TWO)):
            enter(k, *piece)
            leave(k, *piece, True)

    def final(k):
        for part in (ONE, TWO):
            enter(k, *HERE, part)
        for part in (ONE, TWO):
            enter(k, *HERE, part, True)
            collect(k, *HERE, part)
            if k < 3:
                pass_on(k, *HERE, part)

    small(0)
    prepare(0)
    small(1)
    small(2)
    prepare(1)
    chain(0)
    small(3)
    second(0)
    prepare(2)
    chain(1)
    second(1)
    second(2)
    chain(2)
    prepare(3)
    for k in range(3):
        for part in (ONE, TWO):
            sent.append((along(k, *HERE, part, 0)[2], part))
    pl.when(is_end)(lambda: final(0))
    for piece in smalls:
        collect(3, *piece)
    for piece in ((*BY_XY, SMALL_ONE), (*BY_XY, SMALL_TWO), (*BY_Y, SMALL_ONE), (*BY_X, SMALL_TWO)):
        leave(3, *piece)
    pl.when(jnp.logical_not(is_end))(lambda: final(0))
    final(1)
    second(3)
    final(2)
    for piece in ((*BY_X, SMALL_ONE), (*BY_Y, SMALL_TWO)):
        enter(3, *piece)
        leave(3, *piece, True)
    for part in (SMALL_ONE, SMALL_TWO):
        enter(3, *HERE, part)
        enter(3, *HERE, part, True)
    final(3)
    out = pltpu.make_async_copy(acc.at[12], out_ref, out_sem)
    out.start()
    for k in range(4):
        for piece in PIECES + tuple(smalls):
            fetch(k, *piece)[1].wait_send()
    for key, part in sent:
        src = here(0, *HERE, part)
        remote(src, src, send_sem.at[key], z_sem.at[0, 0, 0, 0], p.mate).wait_send()
    out.wait()


def scatter(slots):
    def lands(*lead):
        return jax.ShapeDtypeStruct(lead + (WIN_R, SUB, LANES), jnp.bfloat16)

    any_spec = pl.BlockSpec(memory_space=pl.ANY)
    dma = pltpu.SemaphoreType.DMA
    return pl.pallas_call(
        scatter_kernel,
        out_shape=(lands(), lands(16), lands(4, 3), lands(2, 4, 4)),
        in_specs=[any_spec],
        out_specs=(any_spec,) * 4,
        scratch_shapes=[pltpu.VMEM((16, WIN_R, SUB, LANES), jnp.bfloat16), pltpu.VMEM((WIN_R // 2, SUB, LANES), jnp.bfloat16),
                        dma((16, 3)), dma, dma, dma((44, 4)), dma((16, 3)), dma((4, 3, 4)), dma((2, 4, 4, 3))],
        compiler_params=pltpu.CompilerParams(collective_id=2, has_side_effects=True, vmem_limit_bytes=56 << 20),
    )(slots)[0]


BUFS = 6


def move_kernel(moves, n_in, n_out, *refs):
    ins, outs = refs[:n_in], refs[n_in:n_in + n_out]
    buf, in_sem, out_sem = refs[n_in + n_out:]

    def read(n):
        src, a, _, _, count = moves[n]
        return pltpu.make_async_copy(ins[src].at[pl.ds(a, count)], buf.at[n % BUFS, pl.ds(0, count)], in_sem.at[n % BUFS])

    def write(n):
        _, _, dst, b, count = moves[n]
        return pltpu.make_async_copy(buf.at[n % BUFS, pl.ds(0, count)], outs[dst].at[pl.ds(b, count)], out_sem.at[n % BUFS])

    ahead = BUFS // 2
    for n in range(len(moves) + ahead):
        if n < len(moves):
            if n >= BUFS:
                write(n - BUFS).wait()
            read(n).start()
        if n >= ahead:
            read(n - ahead).wait()
            write(n - ahead).start()
    for n in range(max(0, len(moves) - BUFS), len(moves)):
        write(n).wait()


def move(moves, arrays, out_tiles):
    moves = tuple(m[:1] + (m[1] + c,) + m[2:3] + (m[3] + c, min(BLOCK, m[4] - c)) for m in moves for c in range(0, m[4], BLOCK))
    return pl.pallas_call(
        functools.partial(move_kernel, moves, len(arrays), len(out_tiles)),
        out_shape=tuple(jax.ShapeDtypeStruct((n, SUB, LANES), jnp.bfloat16) for n in out_tiles),
        in_specs=[pl.BlockSpec(memory_space=pl.ANY)] * len(arrays),
        out_specs=(pl.BlockSpec(memory_space=pl.ANY),) * len(out_tiles),
        scratch_shapes=[pltpu.VMEM((BUFS, BLOCK, SUB, LANES), jnp.bfloat16), pltpu.SemaphoreType.DMA((BUFS,)),
                        pltpu.SemaphoreType.DMA((BUFS,))],
        compiler_params=pltpu.CompilerParams(vmem_limit_bytes=20 << 20),
        cost_estimate=pl.CostEstimate(flops=100000000, bytes_accessed=176000000, transcendentals=0),
    )(*arrays)


BLOCK = 704


def norm_kernel(part_ref, out_ref, held, land, send_sem, recv_sem):
    me = lax.axis_index('dp')
    peers = [me + bit * (1 - 2 * ((me // bit) % 2)) for bit in (1, 2, 4, 8, 16)]
    barrier = pltpu.get_barrier_semaphore()
    for peer in peers:
        pl.semaphore_signal(barrier, inc=1, device_id=(peer,), device_id_type=pl.DeviceIdType.MESH)
    pl.semaphore_wait(barrier, 5)
    held[0] = part_ref[...]
    for n, peer in enumerate(peers):
        copy = pltpu.make_async_remote_copy(
            src_ref=held.at[n], dst_ref=land.at[n], send_sem=send_sem.at[n], recv_sem=recv_sem.at[n],
            device_id=(peer,), device_id_type=pl.DeviceIdType.MESH)
        copy.start()
        copy.wait()
        if n < 4:
            held[n + 1] = held[n] + land[n]
        else:
            out_ref[...] = held[n] + land[n]


def sum_over_devices(part):
    vmem = pl.BlockSpec(memory_space=pltpu.VMEM)
    rounds = pltpu.VMEM((5, SUB, LANES), F32)
    total = pl.pallas_call(
        norm_kernel,
        out_shape=jax.ShapeDtypeStruct((SUB, LANES), F32),
        in_specs=[vmem], out_specs=vmem,
        scratch_shapes=[rounds, rounds] + [pltpu.SemaphoreType.DMA((5,))] * 2,
        compiler_params=pltpu.CompilerParams(collective_id=3, has_side_effects=True, vmem_limit_bytes=4 << 20),
    )(jnp.full((SUB, LANES), part, F32))
    return total[0, 0]


def turn_kernel(x_ref, o_ref):
    rows = x_ref.shape[0] * 8
    o_ref[...] = x_ref[...].astype(F32).reshape(rows, LANES).T.astype(jnp.bfloat16)


def turned(tiles, rows, cols):
    return pl.pallas_call(
        turn_kernel,
        out_shape=jax.ShapeDtypeStruct((cols, rows), jnp.bfloat16),
        grid=(cols // LANES, rows // 1024),
        in_specs=[pl.BlockSpec((LANES, None, SUB, LANES), lambda j, i: (i, j, 0, 0))],
        out_specs=pl.BlockSpec((LANES, 1024), lambda j, i: (j, i)),
        cost_estimate=pl.CostEstimate(flops=rows * cols, bytes_accessed=4 * rows * cols, transcendentals=0),
    )(tiles.reshape(rows // SUB, cols // LANES, SUB, LANES))


def rope_tables(positions, head_dim):
    half_dim = head_dim // 2
    inv_freq = ROPE_BASE ** (-2.0 * jnp.arange(half_dim, dtype=F32) / head_dim)
    angles = positions.astype(F32)[:, :, None] * inv_freq
    cos_full = jnp.concatenate([jnp.cos(angles), jnp.cos(angles)], axis=-1)[:, :, None, :]
    sin_full = jnp.concatenate([jnp.sin(angles), jnp.sin(angles)], axis=-1)[:, :, None, :]
    return cos_full, sin_full


def rope_apply(values, cos_full, sin_full):
    half_dim = values.shape[-1] // 2
    rotated = jnp.concatenate([-values[..., half_dim:], values[..., :half_dim]], axis=-1)
    return values * cos_full + rotated * sin_full


def rope_back(grad_rot, cos_full, sin_full):
    half_dim = grad_rot.shape[-1] // 2
    scaled = grad_rot * sin_full
    return grad_rot * cos_full + jnp.concatenate([scaled[..., half_dim:], -scaled[..., :half_dim]], axis=-1)


def rms_parts(values):
    inv_rms = lax.rsqrt(jnp.mean(values * values, axis=-1, keepdims=True) + NORM_EPS)
    return inv_rms, values * inv_rms


def rms_back(d_normed, gain_wide, inv_rms, x_hat):
    d_hat = d_normed * gain_wide
    return inv_rms * (d_hat - x_hat * jnp.mean(d_hat * x_hat, axis=-1, keepdims=True))


def local_grads(x_loc, dy_loc, pos_loc, w_list):
    attn_gain, w_query, w_key, w_value, w_out, mlp_gain, w_gate, w_up, w_down = w_list
    num_seqs, seq_len, model_dim = x_loc.shape
    num_heads, head_dim = w_query.shape[1], w_query.shape[2]
    kv_heads = w_key.shape[1]
    group_size = num_heads // kv_heads
    n_tok = num_seqs * seq_len
    wq_flat = w_query.reshape(model_dim, num_heads * head_dim)
    wk_flat = w_key.reshape(model_dim, kv_heads * head_dim)
    wv_flat = w_value.reshape(model_dim, kv_heads * head_dim)
    wo_flat = w_out.reshape(num_heads * head_dim, model_dim)
    dy_flat = dy_loc.reshape(n_tok, model_dim)
    x_wide = x_loc.reshape(n_tok, model_dim).astype(F32)
    inv_one, value_a8 = rms_parts(x_wide)
    gain_one = attn_gain.astype(F32)
    normed = (value_a8 * gain_one).astype(jnp.bfloat16)
    q_pre = jnp.dot(normed, wq_flat, preferred_element_type=F32).reshape(num_seqs, seq_len, num_heads, head_dim)
    k_pre = jnp.dot(normed, wk_flat, preferred_element_type=F32).reshape(num_seqs, seq_len, kv_heads, head_dim)
    v_heads = jnp.dot(normed, wv_flat, preferred_element_type=F32).astype(jnp.bfloat16).reshape(num_seqs, seq_len, kv_heads, head_dim)
    cos_full, sin_full = rope_tables(pos_loc, head_dim)
    q_rot = rope_apply(q_pre, cos_full, sin_full).astype(jnp.bfloat16).reshape(num_seqs, seq_len, kv_heads, group_size, head_dim)
    k_rot = rope_apply(k_pre, cos_full, sin_full).astype(jnp.bfloat16)
    score_scale = head_dim ** -0.5
    scores = jnp.einsum('bqkgd,bskd->bkgqs', q_rot, k_rot, preferred_element_type=F32) * score_scale
    causal = lax.iota(jnp.int32, seq_len)[:, None] >= lax.iota(jnp.int32, seq_len)[None, :]
    attn_probs = jax.nn.softmax(jnp.where(causal, scores, -1e30), axis=-1)
    probs_low = attn_probs.astype(jnp.bfloat16)
    context = jnp.einsum('bkgqs,bskd->bqkgd', probs_low, v_heads, preferred_element_type=F32).astype(jnp.bfloat16)
    context = context.reshape(n_tok, num_heads * head_dim)
    attn_out = jnp.dot(context, wo_flat, preferred_element_type=F32)
    hidden = (x_wide + attn_out).astype(jnp.bfloat16)
    inv_two, array_b8 = rms_parts(hidden.astype(F32))
    gain_two = mlp_gain.astype(F32)
    normed_mlp = (array_b8 * gain_two).astype(jnp.bfloat16)
    gate_pre = jnp.dot(normed_mlp, w_gate, preferred_element_type=F32)
    up_pre = jnp.dot(normed_mlp, w_up, preferred_element_type=F32)
    gate_sig = jax.nn.sigmoid(gate_pre)
    gate_act = gate_pre * gate_sig
    gated_act = (gate_act * up_pre).astype(jnp.bfloat16)
    g_down = jnp.einsum('nf,nd->fd', gated_act, dy_flat, preferred_element_type=F32)
    d_gated = jnp.einsum('nd,fd->nf', dy_flat, w_down, preferred_element_type=F32)
    d_up = (d_gated * gate_act).astype(jnp.bfloat16)
    d_gate = (d_gated * up_pre * gate_sig * (1.0 + gate_pre * (1.0 - gate_sig))).astype(jnp.bfloat16)
    g_gate = jnp.einsum('nd,nf->df', normed_mlp, d_gate, preferred_element_type=F32)
    g_up = jnp.einsum('nd,nf->df', normed_mlp, d_up, preferred_element_type=F32)
    d_normed_mlp = (jnp.einsum('nf,df->nd', d_gate, w_gate, preferred_element_type=F32)
                    + jnp.einsum('nf,df->nd', d_up, w_up, preferred_element_type=F32))
    g_mlp_gain = jnp.sum(d_normed_mlp * array_b8, axis=0)
    d_hidden = rms_back(d_normed_mlp, gain_two, inv_two, array_b8) + dy_flat.astype(F32)
    d_hidden_low = d_hidden.astype(jnp.bfloat16)
    g_out = jnp.einsum('nc,nd->cd', context, d_hidden_low, preferred_element_type=F32)
    d_context = jnp.einsum('nd,cd->nc', d_hidden_low, wo_flat, preferred_element_type=F32).astype(jnp.bfloat16)
    d_context = d_context.reshape(num_seqs, seq_len, kv_heads, group_size, head_dim)
    d_probs = jnp.einsum('bqkgd,bskd->bkgqs', d_context, v_heads, preferred_element_type=F32)
    g_values = jnp.einsum('bkgqs,bqkgd->bskd', probs_low, d_context, preferred_element_type=F32)
    d_scores = (attn_probs * (d_probs - jnp.sum(d_probs * attn_probs, axis=-1, keepdims=True)) * score_scale).astype(jnp.bfloat16)
    d_q_rot = jnp.einsum('bkgqs,bskd->bqkgd', d_scores, k_rot, preferred_element_type=F32).reshape(num_seqs, seq_len, num_heads, head_dim)
    d_k_rot = jnp.einsum('bkgqs,bqkgd->bskd', d_scores, q_rot, preferred_element_type=F32)
    d_q_pre = rope_back(d_q_rot, cos_full, sin_full).astype(jnp.bfloat16).reshape(n_tok, num_heads * head_dim)
    d_k_pre = rope_back(d_k_rot, cos_full, sin_full).astype(jnp.bfloat16).reshape(n_tok, kv_heads * head_dim)
    d_v_pre = g_values.astype(jnp.bfloat16).reshape(n_tok, kv_heads * head_dim)
    g_query = jnp.einsum('nd,nc->dc', normed, d_q_pre, preferred_element_type=F32)
    g_key = jnp.einsum('nd,nc->dc', normed, d_k_pre, preferred_element_type=F32)
    g_value = jnp.einsum('nd,nc->dc', normed, d_v_pre, preferred_element_type=F32)
    d_normed = (jnp.einsum('nc,dc->nd', d_q_pre, wq_flat, preferred_element_type=F32)
                + jnp.einsum('nc,dc->nd', d_k_pre, wk_flat, preferred_element_type=F32)
                + jnp.einsum('nc,dc->nd', d_v_pre, wv_flat, preferred_element_type=F32))
    g_attn_gain = jnp.sum(d_normed * value_a8, axis=0)
    d_x = rms_back(d_normed, gain_one, inv_one, value_a8) + d_hidden
    grad_list = [g_attn_gain, g_query, g_key, g_value, g_out, g_mlp_gain, g_gate, g_up, g_down]
    return d_x.astype(jnp.bfloat16).reshape(num_seqs, seq_len, model_dim), grad_list


def windows(grad_list):
    tiles = [g.astype(jnp.bfloat16).reshape(2, SUB, LANES) if g.ndim == 1 else to_tiles(g.astype(jnp.bfloat16)) for g in grad_list]
    moves = []
    for dev in range(NDEV):
        for mat in range(len(MATS)):
            a, b = overlap(BASE[dev], BASE[dev] + WIN_R, mat)
            if b > a:
                moves.append((mat, a - OFFS[mat], 0, dev * WIN_R + a - BASE[dev], b - a))
    return move(moves, tiles, (NDEV * WIN_R,))[0].reshape(NDEV, WIN_R, SUB, LANES)


def assemble(slots, w_list):
    moves = []
    for dev in range(NDEV):
        for mat in range(len(MATS)):
            a, b = overlap(OWN[dev], OWN[dev + 1], mat)
            if b > a:
                moves.append((0, dev * WIN_A + a - OWN[dev], mat, a - OFFS[mat], b - a))
    tiles = move(moves, [slots.reshape(NDEV * WIN_A, SUB, LANES)], tuple(m[0] for m in MATS))
    out = []
    for mat, weight in enumerate(w_list):
        if weight.ndim == 1:
            out.append(tiles[mat].reshape(weight.shape))
        else:
            cols = MATS[mat][1] * LANES
            rows = weight.size // cols
            if mat in (1, 2, 3):
                flat = turned(tiles[mat], rows, cols)
                out.append(flat.reshape(weight.shape[1:] + weight.shape[:1]).transpose(2, 0, 1))
            else:
                out.append(from_tiles(tiles[mat], rows, cols).reshape(weight.shape))
    return out


def reduce_scatter(grad_list):
    return scatter(windows(grad_list))


def adamw(grad, clip_scale, master, mean, var, first_row):
    clipped = grad * clip_scale
    new_mean = BETA_ONE * mean + (1.0 - BETA_ONE) * clipped
    new_var = BETA_TWO * var + (1.0 - BETA_TWO) * clipped * clipped
    mean_hat = new_mean / (1.0 - BETA_ONE ** STEP_COUNT)
    var_hat = new_var / (1.0 - BETA_TWO ** STEP_COUNT)
    row = first_row + lax.broadcasted_iota(jnp.int32, master.shape, 0)
    gain_two = OFFS[5] * 8
    is_gain = (row < 16) | ((row >= gain_two) & (row < gain_two + 16))
    decays = jnp.where(is_gain, 0.0, WEIGHT_DECAY)
    new_master = master - LEARN_RATE * (mean_hat / (jnp.sqrt(var_hat) + ADAM_EPS) + decays * master)
    return new_master, new_mean, new_var


def update(win, master, mean, var, tab_in, tab_out):
    me = lax.axis_index('dp')
    state = [s.reshape(ROWS, LANES) for s in (master, mean, var)]
    edge = jnp.stack([s[:HALO] for s in state])
    edge = lax.ppermute(edge, 'dp', [(d, d - 1) for d in range(1, NDEV)])
    summed = unpermute(jnp.asarray(tab_in)[me], win)
    grad = summed[HALO:HALO + ROWS] * (1.0 / NDEV)
    grad_edge = summed[HALO + ROWS:2 * HALO + ROWS] * (1.0 / NDEV)
    grad_norm = jnp.sqrt(sum_over_devices(jnp.sum(grad * grad)))
    clip_scale = jnp.minimum(1.0, 1.0 / (grad_norm + 1e-6))
    new_state = adamw(grad, clip_scale, *state, me * ROWS)
    edge_master = adamw(grad_edge, clip_scale, edge[0], edge[1], edge[2], (me + 1) * ROWS)[0]
    shard = permute(jnp.asarray(tab_out)[me], new_state[0], edge_master)
    return [s.reshape(-1) for s in new_state], grad_norm, shard


def solution(mesh):
    tab_in, tab_out = tables()

    def per_device(x_loc, dy_loc, pos_loc, attn_gain, w_query, w_key, w_value, w_out, mlp_gain, w_gate, w_up, w_down, master_loc, mean_loc, var_loc):
        w_list = (attn_gain, w_query, w_key, w_value, w_out, mlp_gain, w_gate, w_up, w_down)
        grad_x, grad_list = local_grads(x_loc, dy_loc, pos_loc, w_list)
        win = reduce_scatter(grad_list)
        new_state, grad_norm, shard = update(win, master_loc, mean_loc, var_loc, tab_in, tab_out)
        new_weights = assemble(gather(shard), w_list)
        return (grad_x,) + tuple(new_weights) + tuple(new_state) + (grad_norm,)

    in_specs = (P('dp'),) * 3 + (P(),) * 9 + (P('dp'),) * 3
    out_specs = (P('dp'),) + (P(),) * 9 + (P('dp'),) * 3 + (P(),)
    return jax.shard_map(per_device, mesh=mesh, in_specs=in_specs, out_specs=out_specs, check_vma=False)
```

```python
import functools
import jax
import jax.numpy as jnp
import numpy as np
from jax import lax
from jax.experimental import pallas as pl
from jax.experimental.pallas import tpu as pltpu
from jax.sharding import PartitionSpec as P

NORM_EPS = 1e-5
ROPE_BASE = 10000.0
LEARN_RATE = 2e-3
BETA_ONE = 0.9
BETA_TWO = 0.95
ADAM_EPS = 1e-8
WEIGHT_DECAY = 0.1
STEP_COUNT = 100

MATS = ((2, 1), (4096, 16), (512, 2), (512, 2), (4096, 16), (2, 1), (11264, 44), (11264, 44), (11264, 16))
SUB, LANES = 8, 128
F32 = jnp.float32
OFFS = tuple(int(o) for o in np.cumsum([0] + [m[0] for m in MATS]))
NDEV = 32
TILES = OFFS[-1]
ROWS = TILES * 8 // NDEV
HALO = 352
WIN_R = 1408
WIN_A = 1376
S_ROWS = 11464
X_ROWS = 11112


def group_of(row):
    tile = row // 8
    mat = max(m for m in range(len(MATS)) if OFFS[m] <= tile)
    per = MATS[mat][1]
    return OFFS[mat] + (tile - OFFS[mat]) // per * per, per


def plan():
    lo, hi, own = [], [], []
    for dev in range(NDEV):
        start, per = group_of(ROWS * dev)
        last, last_per = group_of(ROWS * (dev + 1) - 1)
        lo.append(start)
        hi.append(last + last_per)
        own.append(start if start * SUB == ROWS * dev else start + per)
    own.append(TILES)
    return lo, hi, own


LO, HI, OWN = plan()
BASE = [min(a, TILES - WIN_R) for a in LO]


def overlap(a, b, mat):
    return max(a, OFFS[mat]), min(b, OFFS[mat + 1])


def tables():
    rows_in, rows_out = [], []
    for dev in range(NDEV):
        r_in, r_out = [], []
        for mat, (_, per) in enumerate(MATS):
            a, b = overlap(LO[dev], HI[dev], mat)
            n = max(0, b - a) // per
            r_in += [a - BASE[dev], SUB * a - ROWS * dev + HALO, n] if n else [0, 0, 0]
            a, b = overlap(OWN[dev], OWN[dev + 1], mat)
            n = max(0, b - a) // per
            r_out += [a - OWN[dev], SUB * a - ROWS * dev, n] if n else [0, 0, 0]
        rows_in.append(r_in)
        rows_out.append(r_out)
    return np.array(rows_in, np.int32), np.array(rows_out, np.int32)


def to_tiles(mat2d):
    rows, cols = mat2d.shape
    return mat2d.reshape(rows // SUB, SUB, cols // LANES, LANES).transpose(0, 2, 1, 3).reshape(-1, SUB, LANES)


def from_tiles(tiles, rows, cols):
    return tiles.reshape(rows // SUB, cols // LANES, SUB, LANES).transpose(0, 2, 1, 3).reshape(rows, cols)


def unpermute_kernel(tab, x_ref, o_ref):
    o_ref[0:HALO, :] = jnp.zeros((HALO, LANES), F32)
    o_ref[S_ROWS - HALO - 24:S_ROWS, :] = jnp.zeros((HALO + 24, LANES), F32)
    for mat, (_, per) in enumerate(MATS):
        t0, r0 = tab[3 * mat], tab[3 * mat + 1]

        def body(g, carry, per=per, t0=t0, r0=r0):
            for j in range(per):
                o_ref[pl.ds(r0 + g * (SUB * per) + j, SUB, stride=per), :] = x_ref[t0 + g * per + j].astype(F32)
            return carry

        lax.fori_loop(0, tab[3 * mat + 2], body, 0)


def unpermute(tab, win):
    return pl.pallas_call(
        unpermute_kernel,
        out_shape=jax.ShapeDtypeStruct((S_ROWS, LANES), F32),
        grid_spec=pltpu.PrefetchScalarGridSpec(
            num_scalar_prefetch=1, grid=(1,),
            in_specs=[pl.BlockSpec((WIN_R, SUB, LANES), lambda i, t: (0, 0, 0))],
            out_specs=pl.BlockSpec((S_ROWS, LANES), lambda i, t: (0, 0))),
        compiler_params=pltpu.CompilerParams(vmem_limit_bytes=40 << 20),
        cost_estimate=pl.CostEstimate(flops=4000000, bytes_accessed=9000000, transcendentals=0),
    )(tab, win)


def permute_kernel(tab, x_ref, h_ref, o_ref, s_ref):
    def fill(k, carry):
        at = pl.ds(pl.multiple_of(k * 64, 64), 64)
        s_ref[at, :] = x_ref[at, :]
        return carry

    lax.fori_loop(0, ROWS // 64, fill, 0)
    s_ref[ROWS // 64 * 64:ROWS, :] = x_ref[ROWS // 64 * 64:ROWS, :]
    s_ref[ROWS:ROWS + HALO, :] = h_ref[...]
    for mat, (_, per) in enumerate(MATS):
        t0, r0 = tab[3 * mat], tab[3 * mat + 1]

        def body(g, carry, per=per, t0=t0, r0=r0):
            for j in range(per):
                o_ref[t0 + g * per + j] = s_ref[pl.ds(r0 + g * (SUB * per) + j, SUB, stride=per), :].astype(jnp.bfloat16)
            return carry

        lax.fori_loop(0, tab[3 * mat + 2], body, 0)


def permute(tab, rows, halo):
    return pl.pallas_call(
        permute_kernel,
        out_shape=jax.ShapeDtypeStruct((WIN_A, SUB, LANES), jnp.bfloat16),
        grid_spec=pltpu.PrefetchScalarGridSpec(
            num_scalar_prefetch=1, grid=(1,),
            in_specs=[pl.BlockSpec((ROWS, LANES), lambda i, t: (0, 0)), pl.BlockSpec((HALO, LANES), lambda i, t: (0, 0))],
            out_specs=pl.BlockSpec((WIN_A, SUB, LANES), lambda i, t: (0, 0, 0)),
            scratch_shapes=[pltpu.VMEM((X_ROWS, LANES), F32)]),
        compiler_params=pltpu.CompilerParams(vmem_limit_bytes=40 << 20),
        cost_estimate=pl.CostEstimate(flops=4000000, bytes_accessed=9000000, transcendentals=0),
    )(tab, rows, halo)


SMALL = 152
ONE, TWO, SMALL_ONE, SMALL_TWO, SMALLS = range(5)


def parts_of(total):
    big = total // 2 - SMALL
    return (0, big), (big, big), (2 * big, SMALL), (2 * big + SMALL, SMALL), (2 * big, 2 * SMALL)


class Place:
    def __init__(self):
        me = lax.axis_index('dp')
        self.me = me
        self.core, self.xx, self.yy, self.zz = me % 2, (me // 2) % 2, (me // 4) % 2, me // 8
        self.mate, self.xn = self.at(self.zz, 0, 0, 1), self.at(self.zz, 0, 1, 0)
        self.yn, self.diag = self.at(self.zz, 1, 0, 0), self.at(self.zz, 1, 1, 0)
        self.up, self.down = self.at(self.zz + 1, 0, 0, 0), self.at(self.zz - 1, 0, 0, 0)
        self.has_up, self.has_down = self.zz < 3, self.zz > 0

    def at(self, z, dy, dx, dc):
        y, x, c = (1 - a if d else a for a, d in ((self.yy, dy), (self.xx, dx), (self.core, dc)))
        return ((z * 2 + y) * 2 + x) * 2 + c

    def greet(self):
        barrier = pltpu.get_barrier_semaphore()
        for cond, target in ((None, self.xn), (None, self.yn), (None, self.mate), (self.has_up, self.up), (self.has_down, self.down)):
            guarded(cond, lambda target=target: pl.semaphore_signal(
                barrier, device_id=(target,), device_id_type=pl.DeviceIdType.MESH))
        pl.semaphore_wait(barrier, 3 + self.has_up.astype(jnp.int32) + self.has_down.astype(jnp.int32))


def guarded(cond, body):
    if cond is None:
        body()
    else:
        pl.when(cond)(body)


def both(a, b):
    return b if a is None else a if b is None else jnp.logical_and(a, b)


def remote(src, dst, send, recv, target):
    return pltpu.make_async_remote_copy(src_ref=src, dst_ref=dst, send_sem=send, recv_sem=recv,
                                        device_id=(target,), device_id_type=pl.DeviceIdType.MESH)


PLANE = HERE, BY_X, BY_Y, BY_XY = (0, 0), (0, 1), (1, 0), (1, 1)


def gather_kernel(x_ref, out_ref, own_sem, send_sem, recv_sem):
    p = Place()
    p.greet()
    parts = parts_of(WIN_A)
    sent = []

    def view(slot, part, own=False):
        at = pl.ds(*parts[part])
        return x_ref.at[at] if own else out_ref.at[slot, at]

    def send(slot, part, target, cond=None, onward=None, own=False):
        desc = remote(view(slot, part, own), view(slot, part), send_sem.at[len(sent)], recv_sem.at[slot, part], target)
        sent.append((part, cond, onward))
        guarded(onward, desc.start)

    def arrived(slot, part):
        remote(view(slot, part), view(slot, part), send_sem.at[0], recv_sem.at[slot, part], p.mate).wait_recv()

    own_copy = pltpu.make_async_copy(x_ref, out_ref.at[p.me], own_sem)
    own_copy.start()
    send(p.me, SMALL_ONE, p.xn, own=True)
    send(p.me, SMALL_TWO, p.yn, own=True)
    for part in (ONE, TWO):
        send(p.me, part, p.up, None, p.has_up, True)
        send(p.me, part, p.down, None, p.has_down, True)
        send(p.me, part, p.xn, own=True)
        send(p.me, part, p.yn, own=True)
    send(p.me, SMALL_ONE, p.yn, own=True)
    send(p.me, SMALL_TWO, p.xn, own=True)
    for part in (ONE, TWO, SMALLS):
        send(p.me, part, p.mate, own=True)
    arrived(p.xn, SMALL_ONE)
    send(p.xn, SMALL_ONE, p.yn)
    arrived(p.yn, SMALL_TWO)
    send(p.yn, SMALL_TWO, p.xn)

    def steps(step):
        if step == 0:
            return [(None, p.zz, None, None)]
        return [(p.zz >= step, p.zz - step, p.up, p.has_up), (p.zz + step <= 3, p.zz + step, p.down, p.has_down)]

    def column(step):
        for cond, z, to, onward in steps(step):
            def body():
                slot = p.at(z, *HERE, 0)
                for part in (ONE, TWO):
                    arrived(slot, part)
                    send(slot, part, to, cond, onward)
                    for target in (p.xn, p.yn, p.mate):
                        send(slot, part, target, cond)
            guarded(cond, body)

    def beside(step):
        for cond, z, _, _ in steps(step):
            def body():
                for part in (ONE, TWO):
                    for dy, dx in (BY_X, BY_Y):
                        slot = p.at(z, dy, dx, 0)
                        arrived(slot, part)
                        if dy == part:
                            send(slot, part, p.xn if dy else p.yn, cond)
                        send(slot, part, p.mate, cond)
            guarded(cond, body)

    def across(step):
        for cond, z, _, _ in steps(step):
            def body():
                slot = p.at(z, *BY_XY, 0)
                for part in (ONE, TWO):
                    arrived(slot, part)
                    send(slot, part, p.mate, cond)
            guarded(cond, body)

    def plane():
        for dy, dx in PLANE:
            slot = p.at(p.zz, dy, dx, 0)
            own = dy + dx == 0
            if not own:
                if dy:
                    arrived(slot, SMALL_ONE)
                if dx:
                    arrived(slot, SMALL_TWO)
                send(slot, SMALLS, p.mate)
            send(slot, SMALLS, p.up, None, p.has_up, own)
            send(slot, SMALLS, p.down, None, p.has_down, own)

    def planes(step):
        for cond, z, to, onward in steps(step):
            def body():
                for dy, dx in PLANE:
                    slot = p.at(z, dy, dx, 0)
                    arrived(slot, SMALLS)
                    send(slot, SMALLS, to, cond, onward)
                    send(slot, SMALLS, p.mate, cond)
            guarded(cond, body)

    column(1)
    beside(0)
    column(2)
    plane()
    beside(1)
    across(0)
    column(3)
    planes(1)
    beside(2)
    planes(2)
    across(1)
    beside(3)
    across(2)
    planes(3)
    across(3)

    def drain(k, carry):
        for part in (ONE, TWO, SMALLS):
            arrived(2 * k + 1 - p.core, part)
        return carry

    lax.fori_loop(0, NDEV // 2, drain, 0)
    for k, (part, cond, onward) in enumerate(sent):
        done = remote(view(p.me, part), view(p.me, part), send_sem.at[k], recv_sem.at[p.me, part], p.mate).wait_send
        guarded(both(cond, onward), done)
    own_copy.wait()


def gather(shard):
    dma = pltpu.SemaphoreType.DMA
    return pl.pallas_call(
        gather_kernel,
        out_shape=jax.ShapeDtypeStruct((NDEV, WIN_A, SUB, LANES), jnp.bfloat16),
        in_specs=[pl.BlockSpec(memory_space=pltpu.VMEM)],
        out_specs=pl.BlockSpec(memory_space=pl.ANY),
        scratch_shapes=[dma, dma((200,)), dma((NDEV, 5))],
        compiler_params=pltpu.CompilerParams(collective_id=1, has_side_effects=True, vmem_limit_bytes=16 << 20),
    )(shard)


PIECES = ((*BY_XY, ONE), (*BY_XY, TWO), (*BY_Y, ONE), (*BY_X, TWO), (*BY_X, ONE), (*BY_Y, TWO), (*HERE, ONE), (*HERE, TWO))


def scatter_kernel(src_ref, out_ref, land_mate, land_hop, land_z, acc, tmp, load_sem, tmp_sem, out_sem, send_sem, mate_sem, hop_sem, z_sem):
    p = Place()
    p.greet()
    parts = parts_of(WIN_R)
    sent = []

    low = jnp.minimum(p.zz, 3 - p.zz)
    order = []
    for far, near in ((3, 3), (2, 0), (1, 2)):
        at = jnp.where(low == 0, far, near)
        order.append(jnp.where(p.zz >= 2, 3 - at, at))
    order.append(p.zz)

    def here(k, dy, dx, part):
        return acc.at[k * 4 + dy * 2 + dx, pl.ds(*parts[part])]

    def fetch(k, dy, dx, part):
        at, i = pl.ds(*parts[part]), k * 4 + dy * 2 + dx
        own = pltpu.make_async_copy(src_ref.at[p.at(order[k], dy, dx, 0), at], here(k, dy, dx, part), load_sem.at[i, min(part, 2)])
        give = remote(src_ref.at[p.at(order[k], dy, dx, 1), at], land_mate.at[i, at], send_sem.at[i, min(part, 2)], mate_sem.at[i, min(part, 2)], p.mate)
        return own, give, land_mate.at[i, at]

    def add(k, dy, dx, part, landed):
        start, count = parts[part]
        copy = pltpu.make_async_copy(landed, tmp.at[pl.ds(0, count)], tmp_sem)
        copy.start()
        copy.wait()
        i = k * 4 + dy * 2 + dx

        def body(t, carry):
            at, to = pl.ds(t * SUB, SUB), pl.ds(start + t * SUB, SUB)
            acc[i, to] = (acc[i, to].astype(F32) + tmp[at].astype(F32)).astype(jnp.bfloat16)
            return carry

        lax.fori_loop(0, count // SUB, body, 0)

    def begin(k, pieces):
        for piece in pieces:
            own, give, _ = fetch(k, *piece)
            give.start()
            own.start()

    def join(k, piece):
        own, give, landed = fetch(k, *piece)
        own.wait()
        give.wait_recv()
        add(k, *piece, landed)

    def hop(k, dy, dx, part, second):
        by_y = (part in (ONE, SMALL_ONE)) != second
        to_dy, to_dx = (0, dx) if by_y else (dy, 0)
        n = to_dy + to_dx + 2 * second
        dst = land_hop.at[k, n, pl.ds(*parts[part])]
        desc = remote(here(k, dy, dx, part), dst, send_sem.at[16 + k * 3 + n, part], hop_sem.at[k, n, part], p.yn if by_y else p.xn)
        return desc, dst, (16 + k * 3 + n, part)

    def leave(k, dy, dx, part, second=False):
        desc, _, key = hop(k, dy, dx, part, second)
        sent.append((key, part))
        desc.start()

    def enter(k, dy, dx, part, second=False):
        by_y = (part in (ONE, SMALL_ONE)) != second
        frm = (1, dx) if by_y else (dy, 1)
        desc, landed, _ = hop(k, *frm, part, second)
        desc.wait_recv()
        add(k, dy, dx, part, landed)

    def along(k, dy, dx, part, way):
        n = dy * 2 + dx
        at = pl.ds(*parts[part])
        key = (28 + k * 4 + n, min(part, 2))
        return remote(here(k, dy, dx, part), land_z.at[way, order[k], n, at], send_sem.at[key], z_sem.at[way, order[k], n, min(part, 2)],
                      p.down if way else p.up), land_z.at[way, order[k], n, at], key

    def collect(k, dy, dx, part):
        for way, cond in ((0, (order[k] >= p.zz) & p.has_down), (1, (order[k] <= p.zz) & p.has_up)):
            @pl.when(cond)
            def _():
                desc, landed, _ = along(k, dy, dx, part, way)
                desc.wait_recv()
                add(k, dy, dx, part, landed)

    def pass_on(k, dy, dx, part):
        for way, cond in ((0, order[k] > p.zz), (1, order[k] < p.zz)):
            @pl.when(cond)
            def _():
                along(k, dy, dx, part, way)[0].start()

    smalls = [(dy, dx, SMALLS) for dy, dx in PLANE]
    begin(0, smalls)
    begin(0, PIECES)
    begin(1, smalls)
    begin(2, smalls)
    begin(1, PIECES)
    begin(2, PIECES)
    begin(3, smalls)
    begin(3, PIECES)

    is_end = low == 0

    def small(k):
        for piece in smalls:
            join(k, piece)
        if k < 3:
            for piece in smalls:
                sent.append((along(k, *piece, 0)[2], SMALLS))
            pl.when(is_end)(lambda: [pass_on(k, *piece) for piece in smalls] and None)

    def chain(k):
        @pl.when(jnp.logical_not(is_end))
        def _():
            for piece in smalls:
                collect(k, *piece)
                pass_on(k, *piece)

    def prepare(k):
        for piece in PIECES:
            join(k, piece)
            if piece[piece[2]] == 1:
                leave(k, *piece)

    def second(k):
        for piece in ((*BY_X, ONE), (*BY_Y, TWO)):
            enter(k, *piece)
            leave(k, *piece, True)

    def final(k):
        for part in (ONE, TWO):
            enter(k, *HERE, part)
        for part in (ONE, TWO):
            enter(k, *HERE, part, True)
            collect(k, *HERE, part)
            if k < 3:
                pass_on(k, *HERE, part)

    small(0)
    prepare(0)
    small(1)
    small(2)
    prepare(1)
    chain(0)
    small(3)
    second(0)
    prepare(2)
    chain(1)
    second(1)
    second(2)
    chain(2)
    prepare(3)
    for k in range(3):
        for part in (ONE, TWO):
            sent.append((along(k, *HERE, part, 0)[2], part))
    pl.when(is_end)(lambda: final(0))
    for piece in smalls:
        collect(3, *piece)
    for piece in ((*BY_XY, SMALL_ONE), (*BY_XY, SMALL_TWO), (*BY_Y, SMALL_ONE), (*BY_X, SMALL_TWO)):
        leave(3, *piece)
    pl.when(jnp.logical_not(is_end))(lambda: final(0))
    final(1)
    second(3)
    final(2)
    for piece in ((*BY_X, SMALL_ONE), (*BY_Y, SMALL_TWO)):
        enter(3, *piece)
        leave(3, *piece, True)
    for part in (SMALL_ONE, SMALL_TWO):
        enter(3, *HERE, part)
        enter(3, *HERE, part, True)
    final(3)
    out = pltpu.make_async_copy(acc.at[12], out_ref, out_sem)
    out.start()
    for k in range(4):
        for piece in PIECES + tuple(smalls):
            fetch(k, *piece)[1].wait_send()
    for key, part in sent:
        src = here(0, *HERE, part)
        remote(src, src, send_sem.at[key], z_sem.at[0, 0, 0, 0], p.mate).wait_send()
    out.wait()


def scatter(slots):
    def lands(*lead):
        return jax.ShapeDtypeStruct(lead + (WIN_R, SUB, LANES), jnp.bfloat16)

    any_spec = pl.BlockSpec(memory_space=pl.ANY)
    dma = pltpu.SemaphoreType.DMA
    return pl.pallas_call(
        scatter_kernel,
        out_shape=(lands(), lands(16), lands(4, 3), lands(2, 4, 4)),
        in_specs=[any_spec],
        out_specs=(any_spec,) * 4,
        scratch_shapes=[pltpu.VMEM((16, WIN_R, SUB, LANES), jnp.bfloat16), pltpu.VMEM((WIN_R // 2, SUB, LANES), jnp.bfloat16),
                        dma((16, 3)), dma, dma, dma((44, 4)), dma((16, 3)), dma((4, 3, 4)), dma((2, 4, 4, 3))],
        compiler_params=pltpu.CompilerParams(collective_id=2, has_side_effects=True, vmem_limit_bytes=56 << 20),
    )(slots)[0]


BUFS = 6


def move_kernel(moves, n_in, n_out, *refs):
    ins, outs = refs[:n_in], refs[n_in:n_in + n_out]
    buf, in_sem, out_sem = refs[n_in + n_out:]

    def read(n):
        src, a, _, _, count = moves[n]
        return pltpu.make_async_copy(ins[src].at[pl.ds(a, count)], buf.at[n % BUFS, pl.ds(0, count)], in_sem.at[n % BUFS])

    def write(n):
        _, _, dst, b, count = moves[n]
        return pltpu.make_async_copy(buf.at[n % BUFS, pl.ds(0, count)], outs[dst].at[pl.ds(b, count)], out_sem.at[n % BUFS])

    ahead = BUFS // 2
    for n in range(len(moves) + ahead):
        if n < len(moves):
            if n >= BUFS:
                write(n - BUFS).wait()
            read(n).start()
        if n >= ahead:
            read(n - ahead).wait()
            write(n - ahead).start()
    for n in range(max(0, len(moves) - BUFS), len(moves)):
        write(n).wait()


def move(moves, arrays, out_tiles):
    moves = tuple(m[:1] + (m[1] + c,) + m[2:3] + (m[3] + c, min(BLOCK, m[4] - c)) for m in moves for c in range(0, m[4], BLOCK))
    return pl.pallas_call(
        functools.partial(move_kernel, moves, len(arrays), len(out_tiles)),
        out_shape=tuple(jax.ShapeDtypeStruct((n, SUB, LANES), jnp.bfloat16) for n in out_tiles),
        in_specs=[pl.BlockSpec(memory_space=pl.ANY)] * len(arrays),
        out_specs=(pl.BlockSpec(memory_space=pl.ANY),) * len(out_tiles),
        scratch_shapes=[pltpu.VMEM((BUFS, BLOCK, SUB, LANES), jnp.bfloat16), pltpu.SemaphoreType.DMA((BUFS,)),
                        pltpu.SemaphoreType.DMA((BUFS,))],
        compiler_params=pltpu.CompilerParams(vmem_limit_bytes=20 << 20),
        cost_estimate=pl.CostEstimate(flops=100000000, bytes_accessed=176000000, transcendentals=0),
    )(*arrays)


BLOCK = 704


def norm_kernel(part_ref, out_ref, held, land, send_sem, recv_sem):
    me = lax.axis_index('dp')
    peers = [me + bit * (1 - 2 * ((me // bit) % 2)) for bit in (1, 2, 4, 8, 16)]
    barrier = pltpu.get_barrier_semaphore()
    for peer in peers:
        pl.semaphore_signal(barrier, inc=1, device_id=(peer,), device_id_type=pl.DeviceIdType.MESH)
    pl.semaphore_wait(barrier, 5)
    held[0] = part_ref[...]
    for n, peer in enumerate(peers):
        copy = pltpu.make_async_remote_copy(
            src_ref=held.at[n], dst_ref=land.at[n], send_sem=send_sem.at[n], recv_sem=recv_sem.at[n],
            device_id=(peer,), device_id_type=pl.DeviceIdType.MESH)
        copy.start()
        copy.wait()
        if n < 4:
            held[n + 1] = held[n] + land[n]
        else:
            out_ref[...] = held[n] + land[n]


def sum_over_devices(part):
    vmem = pl.BlockSpec(memory_space=pltpu.VMEM)
    rounds = pltpu.VMEM((5, SUB, LANES), F32)
    total = pl.pallas_call(
        norm_kernel,
        out_shape=jax.ShapeDtypeStruct((SUB, LANES), F32),
        in_specs=[vmem], out_specs=vmem,
        scratch_shapes=[rounds, rounds] + [pltpu.SemaphoreType.DMA((5,))] * 2,
        compiler_params=pltpu.CompilerParams(collective_id=3, has_side_effects=True, vmem_limit_bytes=4 << 20),
    )(jnp.full((SUB, LANES), part, F32))
    return total[0, 0]


TURN = 512


def turn_kernel(x_ref, o_ref):
    for c in range(o_ref.shape[0] // LANES):
        for r in range(o_ref.shape[1] // TURN):
            x = x_ref[r * (TURN // SUB):(r + 1) * (TURN // SUB), c].astype(F32).reshape(TURN, LANES)
            o_ref[c * LANES:(c + 1) * LANES, r * TURN:(r + 1) * TURN] = x.T.astype(jnp.bfloat16)


def turned(tiles, rows, cols):
    wide = min(cols, 2 * LANES)
    return pl.pallas_call(
        turn_kernel,
        out_shape=jax.ShapeDtypeStruct((cols, rows), jnp.bfloat16),
        grid=(cols // wide,),
        in_specs=[pl.BlockSpec((rows // SUB, wide // LANES, SUB, LANES), lambda j: (0, j, 0, 0))],
        out_specs=pl.BlockSpec((wide, rows), lambda j: (j, 0)),
        cost_estimate=pl.CostEstimate(flops=rows * cols, bytes_accessed=4 * rows * cols, transcendentals=0),
    )(tiles.reshape(rows // SUB, cols // LANES, SUB, LANES))


def rope_tables(positions, head_dim):
    half_dim = head_dim // 2
    inv_freq = ROPE_BASE ** (-2.0 * jnp.arange(half_dim, dtype=F32) / head_dim)
    angles = positions.astype(F32)[:, :, None] * inv_freq
    cos_full = jnp.concatenate([jnp.cos(angles), jnp.cos(angles)], axis=-1)[:, :, None, :]
    sin_full = jnp.concatenate([jnp.sin(angles), jnp.sin(angles)], axis=-1)[:, :, None, :]
    return cos_full, sin_full


def rope_apply(values, cos_full, sin_full):
    half_dim = values.shape[-1] // 2
    rotated = jnp.concatenate([-values[..., half_dim:], values[..., :half_dim]], axis=-1)
    return values * cos_full + rotated * sin_full


def rope_back(grad_rot, cos_full, sin_full):
    half_dim = grad_rot.shape[-1] // 2
    scaled = grad_rot * sin_full
    return grad_rot * cos_full + jnp.concatenate([scaled[..., half_dim:], -scaled[..., :half_dim]], axis=-1)


def rms_parts(values):
    inv_rms = lax.rsqrt(jnp.mean(values * values, axis=-1, keepdims=True) + NORM_EPS)
    return inv_rms, values * inv_rms


def rms_back(d_normed, gain_wide, inv_rms, x_hat):
    d_hat = d_normed * gain_wide
    return inv_rms * (d_hat - x_hat * jnp.mean(d_hat * x_hat, axis=-1, keepdims=True))


def local_grads(x_loc, dy_loc, pos_loc, w_list):
    attn_gain, w_query, w_key, w_value, w_out, mlp_gain, w_gate, w_up, w_down = w_list
    num_seqs, seq_len, model_dim = x_loc.shape
    num_heads, head_dim = w_query.shape[1], w_query.shape[2]
    kv_heads = w_key.shape[1]
    group_size = num_heads // kv_heads
    n_tok = num_seqs * seq_len
    wq_flat = w_query.reshape(model_dim, num_heads * head_dim)
    wk_flat = w_key.reshape(model_dim, kv_heads * head_dim)
    wv_flat = w_value.reshape(model_dim, kv_heads * head_dim)
    wo_flat = w_out.reshape(num_heads * head_dim, model_dim)
    dy_flat = dy_loc.reshape(n_tok, model_dim)
    x_wide = x_loc.reshape(n_tok, model_dim).astype(F32)
    inv_one, value_a8 = rms_parts(x_wide)
    gain_one = attn_gain.astype(F32)
    normed = (value_a8 * gain_one).astype(jnp.bfloat16)
    q_pre = jnp.dot(normed, wq_flat, preferred_element_type=F32).reshape(num_seqs, seq_len, num_heads, head_dim)
    k_pre = jnp.dot(normed, wk_flat, preferred_element_type=F32).reshape(num_seqs, seq_len, kv_heads, head_dim)
    v_heads = jnp.dot(normed, wv_flat, preferred_element_type=F32).astype(jnp.bfloat16).reshape(num_seqs, seq_len, kv_heads, head_dim)
    cos_full, sin_full = rope_tables(pos_loc, head_dim)
    q_rot = rope_apply(q_pre, cos_full, sin_full).astype(jnp.bfloat16).reshape(num_seqs, seq_len, kv_heads, group_size, head_dim)
    k_rot = rope_apply(k_pre, cos_full, sin_full).astype(jnp.bfloat16)
    score_scale = head_dim ** -0.5
    scores = jnp.einsum('bqkgd,bskd->bkgqs', q_rot, k_rot, preferred_element_type=F32) * score_scale
    causal = lax.iota(jnp.int32, seq_len)[:, None] >= lax.iota(jnp.int32, seq_len)[None, :]
    attn_probs = jax.nn.softmax(jnp.where(causal, scores, -1e30), axis=-1)
    probs_low = attn_probs.astype(jnp.bfloat16)
    context = jnp.einsum('bkgqs,bskd->bqkgd', probs_low, v_heads, preferred_element_type=F32).astype(jnp.bfloat16)
    context = context.reshape(n_tok, num_heads * head_dim)
    attn_out = jnp.dot(context, wo_flat, preferred_element_type=F32)
    hidden = (x_wide + attn_out).astype(jnp.bfloat16)
    inv_two, array_b8 = rms_parts(hidden.astype(F32))
    gain_two = mlp_gain.astype(F32)
    normed_mlp = (array_b8 * gain_two).astype(jnp.bfloat16)
    gate_pre = jnp.dot(normed_mlp, w_gate, preferred_element_type=F32)
    up_pre = jnp.dot(normed_mlp, w_up, preferred_element_type=F32)
    gate_sig = jax.nn.sigmoid(gate_pre)
    gate_act = gate_pre * gate_sig
    gated_act = (gate_act * up_pre).astype(jnp.bfloat16)
    g_down = jnp.einsum('nf,nd->fd', gated_act, dy_flat, preferred_element_type=F32)
    d_gated = jnp.einsum('nd,fd->nf', dy_flat, w_down, preferred_element_type=F32)
    d_up = (d_gated * gate_act).astype(jnp.bfloat16)
    d_gate = (d_gated * up_pre * gate_sig * (1.0 + gate_pre * (1.0 - gate_sig))).astype(jnp.bfloat16)
    g_gate = jnp.einsum('nd,nf->df', normed_mlp, d_gate, preferred_element_type=F32)
    g_up = jnp.einsum('nd,nf->df', normed_mlp, d_up, preferred_element_type=F32)
    d_normed_mlp = (jnp.einsum('nf,df->nd', d_gate, w_gate, preferred_element_type=F32)
                    + jnp.einsum('nf,df->nd', d_up, w_up, preferred_element_type=F32))
    g_mlp_gain = jnp.sum(d_normed_mlp * array_b8, axis=0)
    d_hidden = rms_back(d_normed_mlp, gain_two, inv_two, array_b8) + dy_flat.astype(F32)
    d_hidden_low = d_hidden.astype(jnp.bfloat16)
    g_out = jnp.einsum('nc,nd->cd', context, d_hidden_low, preferred_element_type=F32)
    d_context = jnp.einsum('nd,cd->nc', d_hidden_low, wo_flat, preferred_element_type=F32).astype(jnp.bfloat16)
    d_context = d_context.reshape(num_seqs, seq_len, kv_heads, group_size, head_dim)
    d_probs = jnp.einsum('bqkgd,bskd->bkgqs', d_context, v_heads, preferred_element_type=F32)
    g_values = jnp.einsum('bkgqs,bqkgd->bskd', probs_low, d_context, preferred_element_type=F32)
    d_scores = (attn_probs * (d_probs - jnp.sum(d_probs * attn_probs, axis=-1, keepdims=True)) * score_scale).astype(jnp.bfloat16)
    d_q_rot = jnp.einsum('bkgqs,bskd->bqkgd', d_scores, k_rot, preferred_element_type=F32).reshape(num_seqs, seq_len, num_heads, head_dim)
    d_k_rot = jnp.einsum('bkgqs,bqkgd->bskd', d_scores, q_rot, preferred_element_type=F32)
    d_q_pre = rope_back(d_q_rot, cos_full, sin_full).astype(jnp.bfloat16).reshape(n_tok, num_heads * head_dim)
    d_k_pre = rope_back(d_k_rot, cos_full, sin_full).astype(jnp.bfloat16).reshape(n_tok, kv_heads * head_dim)
    d_v_pre = g_values.astype(jnp.bfloat16).reshape(n_tok, kv_heads * head_dim)
    g_query = jnp.einsum('nd,nc->dc', normed, d_q_pre, preferred_element_type=F32)
    g_key = jnp.einsum('nd,nc->dc', normed, d_k_pre, preferred_element_type=F32)
    g_value = jnp.einsum('nd,nc->dc', normed, d_v_pre, preferred_element_type=F32)
    d_normed = (jnp.einsum('nc,dc->nd', d_q_pre, wq_flat, preferred_element_type=F32)
                + jnp.einsum('nc,dc->nd', d_k_pre, wk_flat, preferred_element_type=F32)
                + jnp.einsum('nc,dc->nd', d_v_pre, wv_flat, preferred_element_type=F32))
    g_attn_gain = jnp.sum(d_normed * value_a8, axis=0)
    d_x = rms_back(d_normed, gain_one, inv_one, value_a8) + d_hidden
    grad_list = [g_attn_gain, g_query, g_key, g_value, g_out, g_mlp_gain, g_gate, g_up, g_down]
    return d_x.astype(jnp.bfloat16).reshape(num_seqs, seq_len, model_dim), grad_list


def windows(grad_list):
    tiles = [g.astype(jnp.bfloat16).reshape(2, SUB, LANES) if g.ndim == 1 else to_tiles(g.astype(jnp.bfloat16)) for g in grad_list]
    moves = []
    for dev in range(NDEV):
        for mat in range(len(MATS)):
            a, b = overlap(BASE[dev], BASE[dev] + WIN_R, mat)
            if b > a:
                moves.append((mat, a - OFFS[mat], 0, dev * WIN_R + a - BASE[dev], b - a))
    return move(moves, tiles, (NDEV * WIN_R,))[0].reshape(NDEV, WIN_R, SUB, LANES)


def assemble(slots, w_list):
    moves = []
    for dev in range(NDEV):
        for mat in range(len(MATS)):
            a, b = overlap(OWN[dev], OWN[dev + 1], mat)
            if b > a:
                moves.append((0, dev * WIN_A + a - OWN[dev], mat, a - OFFS[mat], b - a))
    tiles = move(moves, [slots.reshape(NDEV * WIN_A, SUB, LANES)], tuple(m[0] for m in MATS))
    out = []
    for mat, weight in enumerate(w_list):
        if weight.ndim == 1:
            out.append(tiles[mat].reshape(weight.shape))
        else:
            cols = MATS[mat][1] * LANES
            rows = weight.size // cols
            if mat in (1, 2, 3):
                flat = turned(tiles[mat], rows, cols)
                out.append(flat.reshape(weight.shape[1:] + weight.shape[:1]).transpose(2, 0, 1))
            else:
                out.append(from_tiles(tiles[mat], rows, cols).reshape(weight.shape))
    return out


def reduce_scatter(grad_list):
    return scatter(windows(grad_list))


def adamw(grad, clip_scale, master, mean, var, first_row):
    clipped = grad * clip_scale
    new_mean = BETA_ONE * mean + (1.0 - BETA_ONE) * clipped
    new_var = BETA_TWO * var + (1.0 - BETA_TWO) * clipped * clipped
    mean_hat = new_mean / (1.0 - BETA_ONE ** STEP_COUNT)
    var_hat = new_var / (1.0 - BETA_TWO ** STEP_COUNT)
    row = first_row + lax.broadcasted_iota(jnp.int32, master.shape, 0)
    gain_two = OFFS[5] * 8
    is_gain = (row < 16) | ((row >= gain_two) & (row < gain_two + 16))
    decays = jnp.where(is_gain, 0.0, WEIGHT_DECAY)
    new_master = master - LEARN_RATE * (mean_hat / (jnp.sqrt(var_hat) + ADAM_EPS) + decays * master)
    return new_master, new_mean, new_var


def update(win, master, mean, var, tab_in, tab_out):
    me = lax.axis_index('dp')
    state = [s.reshape(ROWS, LANES) for s in (master, mean, var)]
    edge = jnp.stack([s[:HALO] for s in state])
    edge = lax.ppermute(edge, 'dp', [(d, d - 1) for d in range(1, NDEV)])
    summed = unpermute(jnp.asarray(tab_in)[me], win)
    grad = summed[HALO:HALO + ROWS] * (1.0 / NDEV)
    grad_edge = summed[HALO + ROWS:2 * HALO + ROWS] * (1.0 / NDEV)
    grad_norm = jnp.sqrt(sum_over_devices(jnp.sum(grad * grad)))
    clip_scale = jnp.minimum(1.0, 1.0 / (grad_norm + 1e-6))
    new_state = adamw(grad, clip_scale, *state, me * ROWS)
    edge_master = adamw(grad_edge, clip_scale, edge[0], edge[1], edge[2], (me + 1) * ROWS)[0]
    shard = permute(jnp.asarray(tab_out)[me], new_state[0], edge_master)
    return [s.reshape(-1) for s in new_state], grad_norm, shard


def solution(mesh):
    tab_in, tab_out = tables()

    def per_device(x_loc, dy_loc, pos_loc, attn_gain, w_query, w_key, w_value, w_out, mlp_gain, w_gate, w_up, w_down, master_loc, mean_loc, var_loc):
        w_list = (attn_gain, w_query, w_key, w_value, w_out, mlp_gain, w_gate, w_up, w_down)
        grad_x, grad_list = local_grads(x_loc, dy_loc, pos_loc, w_list)
        win = reduce_scatter(grad_list)
        new_state, grad_norm, shard = update(win, master_loc, mean_loc, var_loc, tab_in, tab_out)
        new_weights = assemble(gather(shard), w_list)
        return (grad_x,) + tuple(new_weights) + tuple(new_state) + (grad_norm,)

    in_specs = (P('dp'),) * 3 + (P(),) * 9 + (P('dp'),) * 3
    out_specs = (P('dp'),) + (P(),) * 9 + (P('dp'),) * 3 + (P(),)
    return jax.shard_map(per_device, mesh=mesh, in_specs=in_specs, out_specs=out_specs, check_vma=False)
```
